32 devices in a mesh: batch: 4 (over y, z), seq: 8 (over x, core).
Axes of the slice: x: 4, y: 2, z: 2, core: 2. Of those that a mesh axis runs over, the one named last changes fastest.
The devices are a block of a 4x4x8 slice.
Arguments:
- msa_act: bfloat16 [4096, 256, 64], P(('batch', 'seq')), parts along dimension 0
- msa_mask: int32 [4096, 256], P(('batch', 'seq')), parts along dimension 0
- pair_act: bfloat16 [1024, 256, 128], P(('batch', 'seq')), parts along dimension 0
- w_pair_bias: bfloat16 [128, 8], replicated
- w_row_in: bfloat16 [64, 256], replicated
- w_row_out: bfloat16 [64, 64], replicated
- w_col_in: bfloat16 [64, 144], replicated
- w_col_out: bfloat16 [64, 64], replicated
- w_trans_in: bfloat16 [64, 256], replicated
- w_trans_out: bfloat16 [256, 64], replicated
Outputs:
- output: bfloat16 [4096, 256, 64], P('batch', 'seq'), parts along dimension 0
There are 4 independent parts. The reference program is written for one: setup_inputs(seed, part) draws one part's arguments, and reference() takes and returns one part's arrays. A program takes and returns all parts, laid end to end along the dimension named above; an argument that names none is the same for every part.
All inputs are finite; a program needn't handle non-finite values.
Results may differ from the reference program's by a relative error of at most 0.013669.
Values are sent between devices in bfloat16 or wider.
A program may use at most 768 MiB of HBM per device.

```python
import jax
import jax.numpy as jnp
from jax import lax

SEQ_DEV = 128
GROUP_SIZE = 8
NUM_SEQ = 1024
RESIDUES = 256
MSA_CH = 64
PAIR_CH = 128
NUM_HEADS = 8
HEAD_DIM = 8

HEAD_CH = NUM_HEADS * HEAD_DIM
COL_CH = 2 * HEAD_CH + 2 * HEAD_DIM
TRANS_CH = 4 * MSA_CH
TILE_BUDGET = 2 ** 22
LN_EPS = 1.0e-5
MASK_BIG = 1.0e9
MEAN_EPS = 1.0e-10


def draw_weight(base_key, fan_in, fan_out, gain):
    normal = jax.random.normal(base_key, (fan_in, fan_out), jnp.float32)
    return (gain * fan_in ** -0.5 * normal).astype(jnp.bfloat16)


def draw_mask(mask_key):
    key_cls, key_start, key_len = jax.random.split(mask_key, 3)
    shard_class = jax.random.randint(key_cls, (GROUP_SIZE,), 1, 5)
    len_cap = jnp.repeat(shard_class * (RESIDUES // 4), SEQ_DEV)
    starts = jax.random.randint(key_start, (NUM_SEQ,), 0, RESIDUES)
    lengths = jax.random.randint(key_len, (NUM_SEQ,), 1, len_cap + 1)
    lengths = jnp.where(jnp.arange(NUM_SEQ) == 0, RESIDUES, lengths)
    offset = (jnp.arange(RESIDUES)[None, :] - starts[:, None]) % RESIDUES
    return (offset < lengths[:, None]).astype(jnp.int32)


def setup_inputs(seed: int = 0, part: int = 0) -> dict:
    part_key = jax.random.fold_in(jax.random.key(seed), part)
    key_mask, key_shared, key_shard, key_noise, key_pair = jax.random.split(part_key, 5)
    weight_keys = jax.random.split(jax.random.key(seed + 1), 7)
    shared = jax.random.normal(key_shared, (1, RESIDUES, MSA_CH), jnp.float32)
    per_shard = jnp.repeat(jax.random.normal(key_shard, (GROUP_SIZE, RESIDUES, MSA_CH), jnp.float32), SEQ_DEV, axis=0)
    noise_part = jax.random.normal(key_noise, (NUM_SEQ, RESIDUES, MSA_CH), jnp.float32)
    msa_act = (0.7 * shared + 0.7 * per_shard + 0.7 * noise_part).astype(jnp.bfloat16)
    pair_act = jax.random.normal(key_pair, (RESIDUES, RESIDUES, PAIR_CH), jnp.float32).astype(jnp.bfloat16)
    return {
        'msa_act': msa_act,
        'msa_mask': draw_mask(key_mask),
        'pair_act': pair_act,
        'w_pair_bias': draw_weight(weight_keys[0], PAIR_CH, NUM_HEADS, 1.5),
        'w_row_in': draw_weight(weight_keys[1], MSA_CH, 4 * HEAD_CH, 1.0),
        'w_row_out': draw_weight(weight_keys[2], HEAD_CH, MSA_CH, 3.0),
        'w_col_in': draw_weight(weight_keys[3], MSA_CH, COL_CH, 1.5),
        'w_col_out': draw_weight(weight_keys[4], HEAD_CH, MSA_CH, 2.0),
        'w_trans_in': draw_weight(weight_keys[5], MSA_CH, TRANS_CH, 1.4),
        'w_trans_out': draw_weight(weight_keys[6], TRANS_CH, MSA_CH, 1.5),
    }


def layer_norm(x_in):
    x_f32 = x_in.astype(jnp.float32)
    mean_val = jnp.mean(x_f32, axis=-1, keepdims=True)
    centered = x_f32 - mean_val
    var_val = jnp.mean(centered * centered, axis=-1, keepdims=True)
    return (centered * lax.rsqrt(var_val + LN_EPS)).astype(jnp.bfloat16)


def linear(x_in, weight):
    flat_out = jnp.dot(x_in.reshape(-1, x_in.shape[-1]), weight, preferred_element_type=jnp.float32)
    return flat_out.reshape(x_in.shape[:-1] + (weight.shape[-1],))


def pick_tile(n_rows, per_row):
    best_tile = 1
    for candidate in range(1, n_rows + 1):
        if n_rows % candidate == 0 and candidate * per_row <= TILE_BUDGET:
            best_tile = candidate
    return best_tile


def to_tiles(big_array, tile_rows):
    return big_array.reshape((big_array.shape[0] // tile_rows, tile_rows) + big_array.shape[1:])


def row_tile(act_tile, mask_tile, bias_hij, w_row_in, w_row_out):
    n_rows = act_tile.shape[0]
    projected = linear(layer_norm(act_tile), w_row_in).astype(jnp.bfloat16).astype(jnp.float32)
    projected = projected.reshape(n_rows, RESIDUES, 4, NUM_HEADS, HEAD_DIM)
    logits = jnp.einsum('sihd,sjhd->shij', projected[:, :, 0], projected[:, :, 1]) * HEAD_DIM ** -0.5
    logits = logits + bias_hij[None] + mask_tile[:, None, None, :]
    attn_probs = jax.nn.softmax(logits, axis=-1).astype(jnp.bfloat16).astype(jnp.float32)
    attended = jnp.einsum('shij,sjhd->sihd', attn_probs, projected[:, :, 2])
    gated_out = (jax.nn.sigmoid(projected[:, :, 3]) * attended).astype(jnp.bfloat16)
    row_update = linear(gated_out.reshape(n_rows, RESIDUES, HEAD_CH), w_row_out)
    return (act_tile.astype(jnp.float32) + row_update).astype(jnp.bfloat16)


def col_project(act_tile, w_col_in):
    n_rows = act_tile.shape[0]
    projected = linear(layer_norm(act_tile), w_col_in).astype(jnp.bfloat16).astype(jnp.float32)
    queries = projected[:, :, :HEAD_CH].reshape(n_rows, RESIDUES, NUM_HEADS, HEAD_DIM)
    col_keys = projected[:, :, HEAD_CH:HEAD_CH + HEAD_DIM]
    col_vals = projected[:, :, HEAD_CH + HEAD_DIM:HEAD_CH + 2 * HEAD_DIM]
    col_gates = projected[:, :, HEAD_CH + 2 * HEAD_DIM:].reshape(n_rows, RESIDUES, NUM_HEADS, HEAD_DIM)
    return queries, col_keys, col_vals, col_gates


def reference(msa_act, msa_mask, pair_act, w_pair_bias, w_row_in, w_row_out, w_col_in, w_col_out, w_trans_in, w_trans_out):
    mask_f32 = msa_mask.astype(jnp.float32)
    mask_bias = MASK_BIG * (mask_f32 - 1.0)
    pair_bias = linear(layer_norm(pair_act), w_pair_bias).astype(jnp.bfloat16)
    bias_hij = jnp.transpose(pair_bias, (2, 0, 1)).astype(jnp.float32)
    tile_rows = pick_tile(NUM_SEQ, NUM_HEADS * RESIDUES * RESIDUES)

    def row_body(packed):
        return row_tile(packed[0], packed[1], bias_hij, w_row_in, w_row_out)

    after_row = lax.map(row_body, (to_tiles(msa_act, tile_rows), to_tiles(mask_bias, tile_rows)))

    def stats_body(packed):
        projected = col_project(packed[0], w_col_in)
        q_part = jnp.einsum('sn,snhd->nhd', packed[1], projected[0])
        return q_part, projected[1], projected[2]

    q_parts, col_keys, col_vals = lax.map(stats_body, (after_row, to_tiles(mask_f32, tile_rows)))
    mask_count = jnp.sum(mask_f32, axis=0)
    q_mean = (jnp.sum(q_parts, axis=0) / (mask_count + MEAN_EPS)[:, None, None]).astype(jnp.bfloat16).astype(jnp.float32)
    col_logits = jnp.einsum('nhd,snd->snh', q_mean, col_keys.reshape(NUM_SEQ, RESIDUES, HEAD_DIM)) * HEAD_DIM ** -0.5
    col_logits = col_logits + mask_bias[:, :, None]
    col_probs = jax.nn.softmax(col_logits, axis=0)
    col_out = jnp.einsum('snh,snd->nhd', col_probs, col_vals.reshape(NUM_SEQ, RESIDUES, HEAD_DIM))

    def final_body(act_tile):
        projected = col_project(act_tile, w_col_in)
        gated_out = (jax.nn.sigmoid(projected[3]) * col_out[None]).astype(jnp.bfloat16)
        col_update = linear(gated_out.reshape(act_tile.shape[0], RESIDUES, HEAD_CH), w_col_out)
        after_col = (act_tile.astype(jnp.float32) + col_update).astype(jnp.bfloat16)
        hidden = jnp.maximum(linear(layer_norm(after_col), w_trans_in), 0.0).astype(jnp.bfloat16)
        return (after_col.astype(jnp.float32) + linear(hidden, w_trans_out)).astype(jnp.bfloat16)

    return lax.map(final_body, after_row).reshape(NUM_SEQ, RESIDUES, MSA_CH)
```

```python
import functools

import jax
import jax.numpy as jnp
import numpy as np
from jax import lax
from jax.experimental import pallas as pl
from jax.experimental.pallas import tpu as pltpu
from jax.sharding import PartitionSpec as P

LN_EPS = 1.0e-5
MASK_BIG = 1.0e9
MEAN_EPS = 1.0e-10
LOG2E = 1.4426950408889634
BF = jnp.bfloat16
F32 = jnp.float32
MESH = pl.DeviceIdType.MESH

TILE_PAIRS = 8
LOOP_PAIRS = 2
HEADS_AHEAD = 4
NEXT_AT = 2
TILE_RES = 8


def layer_norm(x_in):
    x_f32 = x_in.astype(F32)
    mean_val = jnp.mean(x_f32, axis=-1, keepdims=True)
    centered = x_f32 - mean_val
    var_val = jnp.mean(centered * centered, axis=-1, keepdims=True)
    return (centered * lax.rsqrt(var_val + LN_EPS)).astype(BF)


def norm_rows(x):
    n = x.shape[0]
    mean = jnp.sum(x, axis=0, keepdims=True) * (1.0 / n)
    centered = x - mean
    var = jnp.sum(centered * centered, axis=0, keepdims=True) * (1.0 / n)
    return (centered * lax.rsqrt(var + LN_EPS)).astype(BF)


def dot(a, b):
    return lax.dot_general(a, b, (((1,), (0,)), ((), ())), preferred_element_type=F32)


def dot_nt(a, b):
    return lax.dot_general(a, b, (((1,), (1,)), ((), ())), preferred_element_type=F32)


def split_bf16(value, parts):
    out, rest = [], np.float64(value)
    for _ in range(parts):
        part = np.float64(np.asarray(rest, np.float32).astype(np.dtype(BF)))
        out.append(float(part))
        rest = rest - part
    return out


def row_prologue(x_bf, m_row, w_in_t, width, n_heads):
    head_dim = width // n_heads
    x = x_bf.astype(F32)
    proj = dot(w_in_t, norm_rows(x)).astype(BF)
    q = proj[:width].astype(F32) * (head_dim ** -0.5 * LOG2E)
    q_hi = q.astype(BF)
    q_lo = (q - q_hi.astype(F32)).astype(BF)
    k = proj[width:2 * width]
    v = proj[2 * width:3 * width].astype(F32)
    gate = jax.nn.sigmoid(proj[3 * width:].astype(F32))
    m_rows = jnp.broadcast_to(m_row - 1.0, (16, x.shape[1])).astype(BF)
    keys = jnp.concatenate([k, k, m_rows], axis=0).T
    return dict(x=x, q_hi=q_hi, q_lo=q_lo, v=v, gate=gate, keys=keys)


def row_stream(loads, w_in_t, w_out_t, bias_ref, n_heads, emit):
    width = w_out_t.shape[1]
    d = width // n_heads
    state = {}

    def start(i):
        if i < len(loads) and i not in state:
            state[i] = row_prologue(*loads[i](), w_in_t, width, n_heads)

    start(0)
    n_res = state[0]['x'].shape[1]
    mask_terms = split_bf16(MASK_BIG * LOG2E, 3)
    row_id = lax.broadcasted_iota(jnp.int32, (16, n_res), 0)
    mask_rows = jnp.zeros((16, n_res), F32)
    for n, term in enumerate(mask_terms):
        mask_rows = jnp.where(row_id == n, term, mask_rows)
    mask_rows = mask_rows.astype(BF)
    head_id = lax.broadcasted_iota(jnp.int32, (width, n_res), 0) // d
    zero = jnp.zeros((width, n_res), BF)
    ones = jnp.ones((8, n_res), F32)

    def logits(i, h):
        mine = head_id == h
        s = state[i]
        rhs = jnp.concatenate([jnp.where(mine, s['q_hi'], zero), jnp.where(mine, s['q_lo'], zero), mask_rows], axis=0)
        return dot(s['keys'], rhs) + bias_ref[h]

    items = [(i, h) for i in range(len(loads)) for h in range(n_heads)]
    pending, heads = {}, {}
    for step in range(len(items) + HEADS_AHEAD):
        if step < len(items):
            i, h = items[step]
            start(i)
            pending[step] = logits(i, h)
            if h == NEXT_AT:
                start(i + 1)
        if step >= HEADS_AHEAD:
            i, h = items[step - HEADS_AHEAD]
            s = state[i]
            t = pending.pop(step - HEADS_AHEAD)
            p = jnp.exp2(t - jnp.max(t, axis=0, keepdims=True)).astype(BF)
            lhs = jnp.concatenate([s['v'][h * d:(h + 1) * d], ones], axis=0).astype(BF)
            o = dot(lhs, p)
            heads.setdefault(i, []).append(o[:d] / o[d:d + 1])
            if h == n_heads - 1:
                gated = (s['gate'] * jnp.concatenate(heads.pop(i), axis=0)).astype(BF)
                emit(i, (s['x'] + dot(w_out_t, gated)).astype(BF))
                del state[i]


def row_kernel(n_dev, e_ref, m_ref, mt_ref, bias_ref, w_in_ref, w_out_ref, recv_ref, mrecv_ref,
               turned, outbox, send_sem, recv_sem, own_sem, msend_sem, mrecv_sem, mown_sem):
    t = pl.program_id(0)
    n_tiles = pl.num_programs(0)
    static_tiles = recv_sem.shape[0]
    me = lax.axis_index('seq')
    n_heads, _, n_res = bias_ref.shape
    pairs = e_ref.shape[1]
    share = n_res // n_dev
    n_local = mt_ref.shape[1]
    chans = turned.shape[1]

    def peer(k):
        return lax.rem(me + k, n_dev)

    def mask_copy(k):
        d = peer(k)
        return pltpu.make_async_remote_copy(
            src_ref=mt_ref.at[pl.ds(pl.multiple_of(d * share, share), share)],
            dst_ref=mrecv_ref.at[:, pl.ds(pl.multiple_of(me * n_local, n_local), n_local)],
            send_sem=msend_sem.at[k], recv_sem=mrecv_sem.at[k], device_id={'seq': d}, device_id_type=MESH)

    def mask_own():
        return pltpu.make_async_copy(
            mt_ref.at[pl.ds(pl.multiple_of(me * share, share), share)],
            mrecv_ref.at[:, pl.ds(pl.multiple_of(me * n_local, n_local), n_local)], mown_sem)

    def tile_copy(tile, k):
        d = peer(k)
        slot = lax.rem(tile, 2)
        return pltpu.make_async_remote_copy(
            src_ref=outbox.at[slot, pl.ds(d * share, share)],
            dst_ref=recv_ref.at[me, :, pl.ds(pl.multiple_of(tile * pairs, pairs), pairs), :],
            send_sem=send_sem.at[slot, k], recv_sem=recv_sem.at[tile, k], device_id={'seq': d}, device_id_type=MESH)

    def tile_own(tile):
        slot = lax.rem(tile, 2)
        return pltpu.make_async_copy(
            outbox.at[slot, pl.ds(me * share, share)],
            recv_ref.at[me, :, pl.ds(pl.multiple_of(tile * pairs, pairs), pairs), :], own_sem.at[slot])

    @pl.when(t == 0)
    def _():
        barrier = pltpu.get_barrier_semaphore()
        for k in range(1, n_dev):
            pl.semaphore_signal(barrier, inc=1, device_id={'seq': peer(k)}, device_id_type=MESH)
        pl.semaphore_wait(barrier, n_dev - 1)
        for k in range(1, n_dev):
            mask_copy(k).start()
        mask_own().start()

    w_in_t = w_in_ref[...]
    w_out_t = w_out_ref[...]

    def body(it, carry):
        def load(u):
            pair = it * LOOP_PAIRS + u // 2
            return lambda: (e_ref[u % 2, pair], m_ref[u % 2, pl.ds(pair, 1), :].astype(F32))

        done = {}

        def emit(u, e1):
            done[u] = e1.astype(F32)
            if u % 2:
                both = jnp.concatenate([done.pop(u - 1), done.pop(u)], axis=0).T
                turned[pl.ds(it * LOOP_PAIRS + u // 2, n_res, stride=pairs), :] = both

        row_stream([load(u) for u in range(2 * LOOP_PAIRS)], w_in_t, w_out_t, bias_ref, n_heads, emit)
        return carry

    lax.fori_loop(0, pairs // LOOP_PAIRS, body, 0)

    @pl.when(t >= 2)
    def _():
        for k in range(1, n_dev):
            tile_copy(t - 2, k).wait_send()
        tile_own(t - 2).wait()

    outbox[lax.rem(t, 2)] = turned[...].reshape(n_res, pairs, chans).astype(BF)
    for k in range(1, n_dev):
        tile_copy(t, k).start()
    tile_own(t).start()

    @pl.when(t == n_tiles - 1)
    def _():
        for tile in range(max(static_tiles - 2, 0), static_tiles):
            for k in range(1, n_dev):
                tile_copy(tile, k).wait_send()
            tile_own(tile).wait()
        for k in range(1, n_dev):
            mask_copy(k).wait_send()
            mask_copy(k).wait_recv()
        mask_own().wait()
        for tile in range(static_tiles):
            for k in range(1, n_dev):
                tile_copy(tile, k).wait_recv()


def row_attention(n_dev, e_t, mask, mask_t, bias_t, w_in_t, w_out_t):
    n_seq, chans, n_res = e_t.shape
    half = n_seq // 2
    tiles = half // TILE_PAIRS
    share = n_res // n_dev
    e_t = e_t.reshape(2, half, chans, n_res)
    mask = mask.reshape(2, half, n_res)

    def whole(a):
        return pl.BlockSpec(a.shape, lambda t: (0,) * a.ndim)

    return pl.pallas_call(
        functools.partial(row_kernel, n_dev),
        grid=(tiles,),
        in_specs=[
            pl.BlockSpec((2, TILE_PAIRS, chans, n_res), lambda t: (0, t, 0, 0)),
            pl.BlockSpec((2, TILE_PAIRS, n_res), lambda t: (0, t, 0)),
            whole(mask_t), whole(bias_t), whole(w_in_t), whole(w_out_t),
        ],
        out_specs=[pl.BlockSpec(memory_space=pl.ANY), pl.BlockSpec(memory_space=pl.ANY)],
        out_shape=[
            jax.ShapeDtypeStruct((n_dev, share, half, 2 * chans), BF),
            jax.ShapeDtypeStruct((share, n_dev * n_seq), F32),
        ],
        scratch_shapes=[
            pltpu.VMEM((n_res * TILE_PAIRS, 2 * chans), F32),
            pltpu.VMEM((2, n_res, TILE_PAIRS, 2 * chans), BF),
            pltpu.SemaphoreType.DMA((2, n_dev)),
            pltpu.SemaphoreType.DMA((tiles, n_dev)),
            pltpu.SemaphoreType.DMA((2,)),
            pltpu.SemaphoreType.DMA((n_dev,)),
            pltpu.SemaphoreType.DMA((n_dev,)),
            pltpu.SemaphoreType.DMA,
        ],
        compiler_params=pltpu.CompilerParams(
            dimension_semantics=('arbitrary',), vmem_limit_bytes=48 * 2 ** 20, collective_id=0, has_side_effects=True),
        name='row_attention',
    )(e_t, mask, mask_t, bias_t, w_in_t, w_out_t)


def col_kernel(n_heads, r_ref, m_ref, wc_ref, wco_ref, wti_ref, wto_ref, o_ref):
    n_dev, n_i, half, lanes = r_ref.shape
    chans = lanes // 2
    width = wco_ref.shape[1]
    d = width // n_heads
    eye = jnp.where(lax.broadcasted_iota(jnp.int32, (lanes, lanes), 0) == lax.broadcasted_iota(jnp.int32, (lanes, lanes), 1),
                    1.0, 0.0).astype(BF)
    low = lax.broadcasted_iota(jnp.int32, (chans, 2 * half), 1) < half
    same_head = (lax.broadcasted_iota(jnp.int32, (width, width), 0) // d
                 == lax.broadcasted_iota(jnp.int32, (width, width), 1) // d)
    state = {}

    def project(i):
        turned = dot_nt(eye, r_ref[:, i].reshape(n_dev * half, lanes))
        cols = []
        for n in range(n_dev // 2):
            a = turned[:chans, n * 2 * half:(n + 1) * 2 * half]
            b = turned[chans:, n * 2 * half:(n + 1) * 2 * half]
            cols.append(jnp.where(low, a, pltpu.roll(b, half, 1)))
            cols.append(jnp.where(low, pltpu.roll(a, half, 1), b))
        x = jnp.concatenate(cols, axis=1)
        state[i] = dict(x=x, proj=dot(wc_ref[...], norm_rows(x)).astype(BF))

    def attend(i):
        proj = state[i]['proj']
        m = m_ref[pl.ds(i, 1), :]
        q_sum = jnp.sum(proj[:width].astype(F32) * m, axis=1, keepdims=True)
        count = jnp.sum(m, axis=1, keepdims=True)
        q_mean = jnp.broadcast_to(q_sum / (count + MEAN_EPS), (width, width))
        q_rows = jnp.where(same_head, q_mean.T, 0.0).astype(BF)
        logits = dot(q_rows, proj[width:2 * width]) * (d ** -0.5) + MASK_BIG * (m - 1.0)
        e = jnp.exp(logits - jnp.max(logits, axis=1, keepdims=True))
        den = jnp.sum(e, axis=1, keepdims=True)
        num = jnp.sum(e * proj[2 * width:3 * width].astype(F32), axis=1, keepdims=True)
        gated = (jax.nn.sigmoid(proj[3 * width:].astype(F32)) * (num / den)).astype(BF)
        state[i]['e2'] = (state[i]['x'] + dot(wco_ref[...], gated)).astype(BF).astype(F32)

    def transition(i):
        e2 = state.pop(i)['e2']
        hidden = jnp.maximum(dot(wti_ref[...], norm_rows(e2)), 0.0).astype(BF)
        o_ref[i] = (e2 + dot(wto_ref[...], hidden)).astype(BF)

    for step in range(n_i + 2):
        if step < n_i:
            project(step)
        if 0 <= step - 1 < n_i:
            attend(step - 1)
        if step >= 2:
            transition(step - 2)


def column_and_transition(n_heads, received, mask, wc, wco, wti, wto):
    n_dev, share, half, lanes = received.shape
    n_seq = mask.shape[1]

    def whole(a):
        return pl.BlockSpec(a.shape, lambda n: (0,) * a.ndim)

    return pl.pallas_call(
        functools.partial(col_kernel, n_heads),
        grid=(share // TILE_RES,),
        in_specs=[
            pl.BlockSpec((n_dev, TILE_RES, half, lanes), lambda n: (0, n, 0, 0)),
            pl.BlockSpec((TILE_RES, n_seq), lambda n: (n, 0)),
            whole(wc), whole(wco), whole(wti), whole(wto),
        ],
        out_specs=pl.BlockSpec((TILE_RES, lanes // 2, n_seq), lambda n: (n, 0, 0)),
        out_shape=jax.ShapeDtypeStruct((share, lanes // 2, n_seq), BF),
        compiler_params=pltpu.CompilerParams(dimension_semantics=('arbitrary',), vmem_limit_bytes=48 * 2 ** 20),
        name='column_and_transition',
    )(received, mask, wc, wco, wti, wto)


def column_weights(w_col_in, width, n_heads):
    d = width // n_heads
    w_t = w_col_in.T
    k = jnp.tile(w_t[width:width + d], (n_heads, 1))
    v = jnp.tile(w_t[width + d:width + 2 * d], (n_heads, 1))
    return jnp.concatenate([w_t[:width], k, v, w_t[width + 2 * d:]], axis=0)


def solution(mesh):
    n_dev = mesh.shape['seq']

    def local_block(msa, mask, pair, w_pair_bias, w_row_in, w_row_out, w_col_in, w_col_out, w_trans_in, w_trans_out):
        n_heads = w_pair_bias.shape[1]
        width = w_col_out.shape[0]
        bias_rows = jnp.einsum('ijc,ch->hij', layer_norm(pair), w_pair_bias, preferred_element_type=F32).astype(BF)
        bias_full = lax.all_gather(bias_rows, 'seq', axis=1, tiled=True)
        bias_t = jnp.transpose(bias_full, (0, 2, 1)).astype(F32) * LOG2E
        received, mask_cols = row_attention(
            n_dev, jnp.transpose(msa, (0, 2, 1)), mask, mask.T.astype(F32), bias_t, w_row_in.T, w_row_out.T)
        out = column_and_transition(
            n_heads, received, mask_cols, column_weights(w_col_in, width, n_heads), w_col_out.T, w_trans_in.T, w_trans_out.T)
        return jnp.transpose(out, (2, 0, 1))

    rows = P(('batch', 'seq'))
    return jax.shard_map(local_block, mesh=mesh, in_specs=(rows, rows, rows) + (P(),) * 7, out_specs=P('batch', 'seq'),
                         check_vma=False)
```

```python
import functools

import jax
import jax.numpy as jnp
import numpy as np
from jax import lax
from jax.experimental import pallas as pl
from jax.experimental.pallas import tpu as pltpu
from jax.sharding import PartitionSpec as P

LN_EPS = 1.0e-5
MASK_BIG = 1.0e9
MEAN_EPS = 1.0e-10
LOG2E = 1.4426950408889634
BF = jnp.bfloat16
F32 = jnp.float32
MESH = pl.DeviceIdType.MESH

TILE_PAIRS = 8
LOOP_PAIRS = 8
HEADS_AHEAD = 5
NEXT_AT = 2
TILE_RES = 8
BIAS_ROWS = 16


def norm_rows(x):
    n = x.shape[0]
    mean = jnp.sum(x, axis=0, keepdims=True) * (1.0 / n)
    centered = x - mean
    var = jnp.sum(centered * centered, axis=0, keepdims=True) * (1.0 / n)
    return (centered * lax.rsqrt(var + LN_EPS)).astype(BF)


def dot(a, b):
    return lax.dot_general(a, b, (((1,), (0,)), ((), ())), preferred_element_type=F32)


def dot_nt(a, b):
    return lax.dot_general(a, b, (((1,), (1,)), ((), ())), preferred_element_type=F32)


def split_bf16(value, parts):
    out, rest = [], np.float64(value)
    for _ in range(parts):
        part = np.float64(np.asarray(rest, np.float32).astype(np.dtype(BF)))
        out.append(float(part))
        rest = rest - part
    return out


def row_prologue(x_bf, m_row, w_in_t, width, n_heads):
    head_dim = width // n_heads
    x = x_bf.astype(F32)
    proj = dot(w_in_t, norm_rows(x)).astype(BF)
    q = proj[:width].astype(F32) * (head_dim ** -0.5 * LOG2E)
    q_hi = q.astype(BF)
    q_lo = (q - q_hi.astype(F32)).astype(BF)
    k = proj[width:2 * width]
    v = proj[2 * width:3 * width].astype(F32)
    gate = jax.nn.sigmoid(proj[3 * width:].astype(F32))
    m_rows = jnp.broadcast_to(m_row - 1.0, (16, x.shape[1])).astype(BF)
    keys = jnp.concatenate([k, k, m_rows], axis=0).T
    return dict(x=x, q_hi=q_hi, q_lo=q_lo, v=v, gate=gate, keys=keys)


def row_stream(loads, w_in_t, w_out_t, bias_ref, n_heads, emit):
    width = w_out_t.shape[1]
    d = width // n_heads
    state = {}

    def start(i):
        if i < len(loads) and i not in state:
            state[i] = row_prologue(*loads[i](), w_in_t, width, n_heads)

    start(0)
    n_res = state[0]['x'].shape[1]
    mask_terms = split_bf16(MASK_BIG * LOG2E, 3)
    row_id = lax.broadcasted_iota(jnp.int32, (16, n_res), 0)
    mask_rows = jnp.zeros((16, n_res), F32)
    for n, term in enumerate(mask_terms):
        mask_rows = jnp.where(row_id == n, term, mask_rows)
    mask_rows = mask_rows.astype(BF)
    per_tile = 16 // d
    sub_id = lax.broadcasted_iota(jnp.int32, (16, n_res), 0) // d
    zero = jnp.zeros((16, n_res), BF)
    ones = jnp.ones((8, n_res), F32)

    def only_head(q, h):
        mine = h // per_tile
        own = jnp.where(sub_id == h % per_tile, q[mine * 16:(mine + 1) * 16], zero)
        return [own if n == mine else zero for n in range(width // 16)]

    def logits(i, h):
        s = state[i]
        rhs = jnp.concatenate(only_head(s['q_hi'], h) + only_head(s['q_lo'], h) + [mask_rows], axis=0)
        return dot(s['keys'], rhs) + bias_ref[h]

    items = [(i, h) for i in range(len(loads)) for h in range(n_heads)]
    pending, heads = {}, {}
    for step in range(len(items) + HEADS_AHEAD):
        if step < len(items):
            i, h = items[step]
            start(i)
            pending[step] = logits(i, h)
            if h == NEXT_AT:
                start(i + 1)
        if step >= HEADS_AHEAD:
            i, h = items[step - HEADS_AHEAD]
            s = state[i]
            t = pending.pop(step - HEADS_AHEAD)
            p = jnp.exp2(t - jnp.max(t, axis=0, keepdims=True)).astype(BF)
            lhs = jnp.concatenate([s['v'][h * d:(h + 1) * d], ones], axis=0).astype(BF)
            o = dot(lhs, p)
            heads.setdefault(i, []).append(o[:d] / o[d:d + 1])
            if h == n_heads - 1:
                gated = (s['gate'] * jnp.concatenate(heads.pop(i), axis=0)).astype(BF)
                emit(i, (s['x'] + dot(w_out_t, gated)).astype(BF))
                del state[i]


def row_kernel(n_dev, e_ref, m_ref, mt_ref, z_ref, w_pair_ref, w_in_ref, w_out_ref, recv_ref, mrecv_ref,
               turned, outbox, bias_rows, bias_all, bias_ref, send_sem, recv_sem, own_sem, msend_sem, mrecv_sem, mown_sem,
               bsend_sem, brecv_sem):
    t = pl.program_id(0)
    n_tiles = pl.num_programs(0)
    static_tiles = recv_sem.shape[0]
    me = lax.axis_index('seq')
    n_heads, _, n_res = bias_ref.shape
    pairs = e_ref.shape[1]
    share = n_res // n_dev
    n_local = mt_ref.shape[1]
    chans = turned.shape[1]

    def peer(k):
        return lax.rem(me + k, n_dev)

    def mask_copy(k):
        d = peer(k)
        return pltpu.make_async_remote_copy(
            src_ref=mt_ref.at[pl.ds(pl.multiple_of(d * share, share), share)],
            dst_ref=mrecv_ref.at[:, pl.ds(pl.multiple_of(me * n_local, n_local), n_local)],
            send_sem=msend_sem.at[k], recv_sem=mrecv_sem.at[k], device_id={'seq': d}, device_id_type=MESH)

    def mask_own():
        return pltpu.make_async_copy(
            mt_ref.at[pl.ds(pl.multiple_of(me * share, share), share)],
            mrecv_ref.at[:, pl.ds(pl.multiple_of(me * n_local, n_local), n_local)], mown_sem)

    def tile_copy(tile, k):
        d = peer(k)
        slot = lax.rem(tile, 2)
        return pltpu.make_async_remote_copy(
            src_ref=outbox.at[slot, pl.ds(d * share, share)],
            dst_ref=recv_ref.at[me, :, pl.ds(pl.multiple_of(tile * pairs, pairs), pairs), :],
            send_sem=send_sem.at[slot, k], recv_sem=recv_sem.at[tile, k], device_id={'seq': d}, device_id_type=MESH)

    def tile_own(tile):
        slot = lax.rem(tile, 2)
        return pltpu.make_async_copy(
            outbox.at[slot, pl.ds(me * share, share)],
            recv_ref.at[me, :, pl.ds(pl.multiple_of(tile * pairs, pairs), pairs), :], own_sem.at[slot])

    def bias_copy(c, k):
        rows = bias_all.at[:, pl.ds(pl.multiple_of(me * share + c * BIAS_ROWS, BIAS_ROWS), BIAS_ROWS), :]
        return pltpu.make_async_remote_copy(
            src_ref=rows, dst_ref=rows, send_sem=bsend_sem.at[c, k], recv_sem=brecv_sem.at[c, k],
            device_id={'seq': peer(k)}, device_id_type=MESH)

    @pl.when(t == 0)
    def _():
        barrier = pltpu.get_barrier_semaphore()
        for k in range(1, n_dev):
            pl.semaphore_signal(barrier, inc=1, device_id={'seq': peer(k)}, device_id_type=MESH)
        z_ch = z_ref.shape[2]
        eye = jnp.where(lax.broadcasted_iota(jnp.int32, (z_ch, z_ch), 0) == lax.broadcasted_iota(jnp.int32, (z_ch, z_ch), 1),
                        1.0, 0.0).astype(BF)
        w_pair = w_pair_ref[...]
        for c in range(share // BIAS_ROWS):
            def rows_step(n, carry, c=c):
                i = c * BIAS_ROWS + n * 4
                turned_z = dot_nt(eye, z_ref[pl.ds(i, 4)].reshape(4 * n_res, z_ch))
                b = dot(w_pair, norm_rows(turned_z))
                for u in range(4):
                    for part in range(n_res // 128):
                        at = u * n_res + part * 128
                        bias_rows[part, pl.ds(i + u, n_heads, stride=share), :] = b[:, at:at + 128]
                return carry

            lax.fori_loop(0, BIAS_ROWS // 4, rows_step, 0)
            for part in range(n_res // 128):
                own = bias_rows[part].reshape(n_heads, share, 128)[:, c * BIAS_ROWS:(c + 1) * BIAS_ROWS]
                bias_all[:, pl.ds(pl.multiple_of(me * share + c * BIAS_ROWS, BIAS_ROWS), BIAS_ROWS),
                         part * 128:(part + 1) * 128] = own.astype(BF)
            if c == 0:
                pl.semaphore_wait(barrier, n_dev - 1)
            for k in range(1, n_dev):
                bias_copy(c, k).start()
        for k in range(1, n_dev):
            mask_copy(k).start()
        mask_own().start()
        for c in range(share // BIAS_ROWS):
            for k in range(1, n_dev):
                bias_copy(c, k).wait_recv()

        def turn(h, carry):
            bias_ref[h] = bias_all[h].astype(F32).T * LOG2E
            return carry

        lax.fori_loop(0, n_heads, turn, 0)
        for c in range(share // BIAS_ROWS):
            for k in range(1, n_dev):
                bias_copy(c, k).wait_send()

    w_in_t = w_in_ref[...]
    w_out_t = w_out_ref[...]

    def body(it, carry):
        def load(u):
            pair = it * LOOP_PAIRS + u // 2
            return lambda: (e_ref[u % 2, pair], m_ref[u % 2, pl.ds(pair, 1), :].astype(F32))

        done = {}

        def emit(u, e1):
            done[u] = e1.astype(F32)
            if u % 2:
                both = jnp.concatenate([done.pop(u - 1), done.pop(u)], axis=0).T
                turned[pl.ds(it * LOOP_PAIRS + u // 2, n_res, stride=pairs), :] = both

        row_stream([load(u) for u in range(2 * LOOP_PAIRS)], w_in_t, w_out_t, bias_ref, n_heads, emit)
        return carry

    lax.fori_loop(0, pairs // LOOP_PAIRS, body, 0)

    @pl.when(t >= 2)
    def _():
        for k in range(1, n_dev):
            tile_copy(t - 2, k).wait_send()
        tile_own(t - 2).wait()

    outbox[lax.rem(t, 2)] = turned[...].reshape(n_res, pairs, chans).astype(BF)
    for k in range(1, n_dev):
        tile_copy(t, k).start()
    tile_own(t).start()

    @pl.when(t == n_tiles - 1)
    def _():
        for tile in range(max(static_tiles - 2, 0), static_tiles):
            for k in range(1, n_dev):
                tile_copy(tile, k).wait_send()
            tile_own(tile).wait()
        for k in range(1, n_dev):
            mask_copy(k).wait_send()
            mask_copy(k).wait_recv()
        mask_own().wait()
        for tile in range(static_tiles):
            for k in range(1, n_dev):
                tile_copy(tile, k).wait_recv()


def row_attention(n_dev, e_t, mask, mask_t, pair, w_pair_t, w_in_t, w_out_t):
    n_seq, chans, n_res = e_t.shape
    half = n_seq // 2
    tiles = half // TILE_PAIRS
    share = n_res // n_dev
    n_heads = w_pair_t.shape[0]
    e_t = e_t.reshape(2, half, chans, n_res)
    mask = mask.reshape(2, half, n_res)

    def whole(a):
        return pl.BlockSpec(a.shape, lambda t: (0,) * a.ndim)

    return pl.pallas_call(
        functools.partial(row_kernel, n_dev),
        grid=(tiles,),
        in_specs=[
            pl.BlockSpec((2, TILE_PAIRS, chans, n_res), lambda t: (0, t, 0, 0)),
            pl.BlockSpec((2, TILE_PAIRS, n_res), lambda t: (0, t, 0)),
            whole(mask_t), whole(pair), whole(w_pair_t), whole(w_in_t), whole(w_out_t),
        ],
        out_specs=[pl.BlockSpec(memory_space=pl.ANY), pl.BlockSpec(memory_space=pl.ANY)],
        out_shape=[
            jax.ShapeDtypeStruct((n_dev, share, half, 2 * chans), BF),
            jax.ShapeDtypeStruct((share, n_dev * n_seq), F32),
        ],
        scratch_shapes=[
            pltpu.VMEM((n_res * TILE_PAIRS, 2 * chans), F32),
            pltpu.VMEM((2, n_res, TILE_PAIRS, 2 * chans), BF),
            pltpu.VMEM((n_res // 128, n_heads * share, 128), F32),
            pltpu.VMEM((n_heads, n_res, n_res), BF),
            pltpu.VMEM((n_heads, n_res, n_res), F32),
            pltpu.SemaphoreType.DMA((2, n_dev)),
            pltpu.SemaphoreType.DMA((tiles, n_dev)),
            pltpu.SemaphoreType.DMA((2,)),
            pltpu.SemaphoreType.DMA((n_dev,)),
            pltpu.SemaphoreType.DMA((n_dev,)),
            pltpu.SemaphoreType.DMA,
            pltpu.SemaphoreType.DMA((share // BIAS_ROWS, n_dev)),
            pltpu.SemaphoreType.DMA((share // BIAS_ROWS, n_dev)),
        ],
        compiler_params=pltpu.CompilerParams(
            dimension_semantics=('arbitrary',), vmem_limit_bytes=48 * 2 ** 20, collective_id=0, has_side_effects=True),
        name='row_attention',
    )(e_t, mask, mask_t, pair, w_pair_t, w_in_t, w_out_t)


def col_kernel(n_heads, r_ref, m_ref, wc_ref, wco_ref, wti_ref, wto_ref, o_ref):
    n_dev, n_i, half, lanes = r_ref.shape
    chans = lanes // 2
    width = wco_ref.shape[1]
    d = width // n_heads
    eye = jnp.where(lax.broadcasted_iota(jnp.int32, (lanes, lanes), 0) == lax.broadcasted_iota(jnp.int32, (lanes, lanes), 1),
                    1.0, 0.0).astype(BF)
    low = lax.broadcasted_iota(jnp.int32, (chans, 2 * half), 1) < half
    same_head = (lax.broadcasted_iota(jnp.int32, (width, width), 0) // d
                 == lax.broadcasted_iota(jnp.int32, (width, width), 1) // d)
    state = {}

    def project(i):
        turned = dot_nt(eye, r_ref[:, i].reshape(n_dev * half, lanes))
        cols = []
        for n in range(n_dev // 2):
            a = turned[:chans, n * 2 * half:(n + 1) * 2 * half]
            b = turned[chans:, n * 2 * half:(n + 1) * 2 * half]
            cols.append(jnp.where(low, a, pltpu.roll(b, half, 1)))
            cols.append(jnp.where(low, pltpu.roll(a, half, 1), b))
        x = jnp.concatenate(cols, axis=1)
        state[i] = dict(x=x, proj=dot(wc_ref[...], norm_rows(x)).astype(BF))

    def attend(i):
        proj = state[i]['proj']
        m = m_ref[pl.ds(i, 1), :]
        q_sum = jnp.sum(proj[:width].astype(F32) * m, axis=1, keepdims=True)
        count = jnp.sum(m, axis=1, keepdims=True)
        q_mean = jnp.broadcast_to(q_sum / (count + MEAN_EPS), (width, width))
        q_rows = jnp.where(same_head, q_mean.T, 0.0).astype(BF)
        logits = dot(q_rows, proj[width:2 * width]) * (d ** -0.5) + MASK_BIG * (m - 1.0)
        e = jnp.exp(logits - jnp.max(logits, axis=1, keepdims=True))
        den = jnp.sum(e, axis=1, keepdims=True)
        num = jnp.sum(e * proj[2 * width:3 * width].astype(F32), axis=1, keepdims=True)
        gated = (jax.nn.sigmoid(proj[3 * width:].astype(F32)) * (num / den)).astype(BF)
        state[i]['e2'] = (state[i]['x'] + dot(wco_ref[...], gated)).astype(BF).astype(F32)

    def transition(i):
        e2 = state.pop(i)['e2']
        hidden = jnp.maximum(dot(wti_ref[...], norm_rows(e2)), 0.0).astype(BF)
        o_ref[i] = (e2 + dot(wto_ref[...], hidden)).astype(BF)

    for step in range(n_i + 2):
        if step < n_i:
            project(step)
        if 0 <= step - 1 < n_i:
            attend(step - 1)
        if step >= 2:
            transition(step - 2)


def column_and_transition(n_heads, received, mask, wc, wco, wti, wto):
    n_dev, share, half, lanes = received.shape
    n_seq = mask.shape[1]

    def whole(a):
        return pl.BlockSpec(a.shape, lambda n: (0,) * a.ndim)

    return pl.pallas_call(
        functools.partial(col_kernel, n_heads),
        grid=(share // TILE_RES,),
        in_specs=[
            pl.BlockSpec((n_dev, TILE_RES, half, lanes), lambda n: (0, n, 0, 0)),
            pl.BlockSpec((TILE_RES, n_seq), lambda n: (n, 0)),
            whole(wc), whole(wco), whole(wti), whole(wto),
        ],
        out_specs=pl.BlockSpec((TILE_RES, lanes // 2, n_seq), lambda n: (n, 0, 0)),
        out_shape=jax.ShapeDtypeStruct((share, lanes // 2, n_seq), BF),
        compiler_params=pltpu.CompilerParams(dimension_semantics=('arbitrary',), vmem_limit_bytes=48 * 2 ** 20),
        name='column_and_transition',
    )(received, mask, wc, wco, wti, wto)


def column_weights(w_col_in, width, n_heads):
    d = width // n_heads
    w_t = w_col_in.T
    k = jnp.tile(w_t[width:width + d], (n_heads, 1))
    v = jnp.tile(w_t[width + d:width + 2 * d], (n_heads, 1))
    return jnp.concatenate([w_t[:width], k, v, w_t[width + 2 * d:]], axis=0)


def solution(mesh):
    n_dev = mesh.shape['seq']

    def local_block(msa, mask, pair, w_pair_bias, w_row_in, w_row_out, w_col_in, w_col_out, w_trans_in, w_trans_out):
        n_heads = w_pair_bias.shape[1]
        width = w_col_out.shape[0]
        received, mask_cols = row_attention(
            n_dev, jnp.transpose(msa, (0, 2, 1)), mask, mask.T.astype(F32), pair, w_pair_bias.T, w_row_in.T, w_row_out.T)
        out = column_and_transition(
            n_heads, received, mask_cols, column_weights(w_col_in, width, n_heads), w_col_out.T, w_trans_in.T, w_trans_out.T)
        return jnp.transpose(out, (2, 0, 1))

    rows = P(('batch', 'seq'))
    return jax.shard_map(local_block, mesh=mesh, in_specs=(rows, rows, rows) + (P(),) * 7, out_specs=P('batch', 'seq'),
                         check_vma=False)
```

```python
import functools

import jax
import jax.numpy as jnp
import numpy as np
from jax import lax
from jax.experimental import pallas as pl
from jax.experimental.pallas import tpu as pltpu
from jax.sharding import PartitionSpec as P

LN_EPS = 1.0e-5
MASK_BIG = 1.0e9
MEAN_EPS = 1.0e-10
LOG2E = 1.4426950408889634
BF = jnp.bfloat16
F32 = jnp.float32
MESH = pl.DeviceIdType.MESH

VMEM_BYTES = 67_043_328

TILE_PAIRS = 8
ROW_TIME = dict(norm=-6, project=-5, split=-3, logits=0, softmax=4, values=5, divide=8, gate=9, out=10, emit=11)
ROW_ORDER = ('logits', 'values', 'project', 'out', 'softmax', 'norm', 'split', 'divide', 'gate', 'emit')
TILE_RES = 16
COL_STAGES = (('finish', 5), ('hidden', 4), ('out', 3), ('logits', 2), ('project', 1), ('turn', 0), ('softmax', 2), ('q_mean', 1))
BIAS_ROWS = 16


def norm_rows(x):
    n = x.shape[0]
    mean = jnp.sum(x, axis=0, keepdims=True) * (1.0 / n)
    centered = x - mean
    var = jnp.sum(centered * centered, axis=0, keepdims=True) * (1.0 / n)
    return (centered * lax.rsqrt(var + LN_EPS)).astype(BF)


def dot(a, b):
    return lax.dot_general(a, b, (((1,), (0,)), ((), ())), preferred_element_type=F32)


def dot_nt(a, b):
    return lax.dot_general(a, b, (((1,), (1,)), ((), ())), preferred_element_type=F32)


def split_bf16(value, parts):
    out, rest = [], np.float64(value)
    for _ in range(parts):
        part = np.float64(np.asarray(rest, np.float32).astype(np.dtype(BF)))
        out.append(float(part))
        rest = rest - part
    return out


def transposed(w):
    return w.astype(F32).T.astype(BF)


def row_stream(loads, w_in_t, w_out_t, bias_ref, n_heads, n_res, emit):
    width = w_out_t.shape[1]
    d = width // n_heads
    row_id = lax.broadcasted_iota(jnp.int32, (16, n_res), 0)
    mask_rows = jnp.zeros((16, n_res), F32)
    for n, term in enumerate(split_bf16(MASK_BIG * LOG2E, 3)):
        mask_rows = jnp.where(row_id == n, term, mask_rows)
    mask_rows = mask_rows.astype(BF)
    per_tile = 16 // d
    zero = jnp.zeros((16, n_res), BF)
    ones = jnp.ones((8, n_res), F32)
    state = [dict() for _ in loads]

    def norm(i, h):
        x_bf, m_row = loads[i]()
        x = x_bf.astype(F32)
        state[i].update(x=x, m_row=m_row, y=norm_rows(x))

    def project(i, h):
        state[i]['proj'] = dot(w_in_t, state[i].pop('y')).astype(BF)

    def split(i, h):
        s = state[i]
        proj = s.pop('proj')
        q = proj[:width].astype(F32) * (d ** -0.5 * LOG2E)
        q_hi = q.astype(BF)
        k = proj[width:2 * width]
        m_rows = jnp.broadcast_to(s.pop('m_row') - 1.0, (16, n_res)).astype(BF)
        s.update(q_hi=q_hi, q_lo=(q - q_hi.astype(F32)).astype(BF), v=proj[2 * width:3 * width], g=proj[3 * width:],
                 keys=jnp.concatenate([k, k, m_rows], axis=0).T)

    def only_head(q, h):
        mine = h // per_tile
        own = jnp.where(row_id // d == h % per_tile, q[mine * 16:(mine + 1) * 16], zero)
        return [own if n == mine else zero for n in range(width // 16)]

    def logits(i, h):
        s = state[i]
        rhs = jnp.concatenate(only_head(s['q_hi'], h) + only_head(s['q_lo'], h) + [mask_rows], axis=0)
        s['t', h] = dot(s['keys'], rhs) + bias_ref[h]

    def softmax(i, h):
        t = state[i].pop(('t', h))
        state[i]['p', h] = jnp.exp2(t - jnp.max(t, axis=0, keepdims=True)).astype(BF)

    def values(i, h):
        s = state[i]
        lhs = jnp.concatenate([s['v'][h * d:(h + 1) * d].astype(F32), ones], axis=0).astype(BF)
        s['o', h] = dot(lhs, s.pop(('p', h)))

    def divide(i, h):
        o = state[i].pop(('o', h))
        state[i]['r', h] = o[:d] / o[d:d + 8]

    def gate(i, h):
        s = state[i]
        o = jnp.concatenate([s.pop(('r', n)) for n in range(n_heads)], axis=0)
        s['gated'] = (jax.nn.sigmoid(s.pop('g').astype(F32)) * o).astype(BF)

    def out(i, h):
        state[i]['u'] = dot(w_out_t, state[i].pop('gated'))

    def last(i, h):
        s = state[i]
        emit(i, (s.pop('x') + s.pop('u')).astype(BF))
        s.clear()

    stages = dict(norm=norm, project=project, split=split, logits=logits, softmax=softmax, values=values, divide=divide,
                  gate=gate, out=out, emit=last)
    first, end = ('norm', 'project', 'split'), ('gate', 'out', 'emit')
    events = []
    for i in range(len(loads)):
        for rank, name in enumerate(ROW_ORDER):
            heads = [0] if name in first else [n_heads - 1] if name in end else range(n_heads)
            events += [(n_heads * i + h + ROW_TIME[name], rank, i, h, name) for h in heads]
    for _, _, i, h, name in sorted(events):
        stages[name](i, h)


def row_kernel(n_dev, e_ref, m_ref, z_hbm, w_pair_ref, w_in_ref, w_out_ref, recv_ref, mrecv_ref,
               turned, outbox, z_ref, mt_ref, bias_rows, bias_all, bias_ref, send_sem, recv_sem, own_sem, msend_sem, mrecv_sem,
               mown_sem, z_sem, bsend_sem, brecv_sem, fsend_sem, frecv_sem):
    t = pl.program_id(0)
    n_tiles = pl.num_programs(0)
    static_tiles = recv_sem.shape[0]
    me = lax.axis_index('seq')
    n_heads, _, n_res = bias_ref.shape
    pairs = e_ref.shape[1]
    share = n_res // n_dev
    n_local = mt_ref.shape[1]
    chans = turned.shape[1]

    def peer(k):
        return lax.rem(me + k, n_dev)

    def mask_copy(k):
        d = peer(k)
        return pltpu.make_async_remote_copy(
            src_ref=mt_ref.at[pl.ds(pl.multiple_of(d * share, share), share)],
            dst_ref=mrecv_ref.at[:, pl.ds(pl.multiple_of(me * n_local, n_local), n_local)],
            send_sem=msend_sem.at[k], recv_sem=mrecv_sem.at[k], device_id={'seq': d}, device_id_type=MESH)

    def mask_own():
        return pltpu.make_async_copy(
            mt_ref.at[pl.ds(pl.multiple_of(me * share, share), share)],
            mrecv_ref.at[:, pl.ds(pl.multiple_of(me * n_local, n_local), n_local)], mown_sem)

    def tile_copy(tile, k):
        d = peer(k)
        slot = lax.rem(tile, 2)
        return pltpu.make_async_remote_copy(
            src_ref=outbox.at[slot, pl.ds(d * share, share)],
            dst_ref=recv_ref.at[me, :, pl.ds(pl.multiple_of(tile * pairs, pairs), pairs), :],
            send_sem=send_sem.at[slot, k], recv_sem=recv_sem.at[tile, k], device_id={'seq': d}, device_id_type=MESH)

    def tile_own(tile):
        slot = lax.rem(tile, 2)
        return pltpu.make_async_copy(
            outbox.at[slot, pl.ds(me * share, share)],
            recv_ref.at[me, :, pl.ds(pl.multiple_of(tile * pairs, pairs), pairs), :], own_sem.at[slot])

    chunks = share // BIAS_ROWS
    others = n_dev // 2
    partner = me + 1 - 2 * lax.rem(me, 2)

    def bias_block(owner, c):
        return bias_all.at[:, pl.ds(pl.multiple_of(owner * share + c * BIAS_ROWS, BIAS_ROWS), BIAS_ROWS), :]

    def bias_copy(c, q):
        to = partner if q == 0 else lax.rem(me + 2 * q, n_dev)
        return pltpu.make_async_remote_copy(
            src_ref=bias_block(me, c), dst_ref=bias_block(me, c), send_sem=bsend_sem.at[c, q], recv_sem=brecv_sem.at[c, q],
            device_id={'seq': to}, device_id_type=MESH)

    def bias_forward(c, q):
        owner = lax.rem(me + n_dev - 2 * q, n_dev)
        return pltpu.make_async_remote_copy(
            src_ref=bias_block(owner, c), dst_ref=bias_block(owner, c), send_sem=fsend_sem.at[c, q],
            recv_sem=frecv_sem.at[c, q], device_id={'seq': partner}, device_id_type=MESH)

    def z_copy(c):
        rows = pl.ds(c * BIAS_ROWS, BIAS_ROWS)
        return pltpu.make_async_copy(z_hbm.at[rows], z_ref.at[rows], z_sem.at[c])

    @pl.when(t == 0)
    def _():
        for c in range(chunks):
            z_copy(c).start()
        barrier = pltpu.get_barrier_semaphore()
        for k in range(1, n_dev):
            pl.semaphore_signal(barrier, inc=1, device_id={'seq': peer(k)}, device_id_type=MESH)
        z_ch = z_ref.shape[2]
        eye = jnp.where(lax.broadcasted_iota(jnp.int32, (z_ch, z_ch), 0) == lax.broadcasted_iota(jnp.int32, (z_ch, z_ch), 1),
                        1.0, 0.0).astype(BF)
        w_pair = w_pair_ref[...]
        for c in range(chunks):
            z_copy(c).wait()

            def rows_step(n, carry, c=c):
                i = c * BIAS_ROWS + n * 4
                turned_z = dot_nt(eye, z_ref[pl.ds(i, 4)].reshape(4 * n_res, z_ch))
                b = dot(w_pair, norm_rows(turned_z))
                for u in range(4):
                    for part in range(n_res // 128):
                        at = u * n_res + part * 128
                        bias_rows[part, pl.ds(i + u, n_heads, stride=share), :] = b[:, at:at + 128]
                return carry

            lax.fori_loop(0, BIAS_ROWS // 4, rows_step, 0)
            for part in range(n_res // 128):
                own = bias_rows[part].reshape(n_heads, share, 128)[:, c * BIAS_ROWS:(c + 1) * BIAS_ROWS]
                bias_all[:, pl.ds(pl.multiple_of(me * share + c * BIAS_ROWS, BIAS_ROWS), BIAS_ROWS),
                         part * 128:(part + 1) * 128] = own.astype(BF)
            if c == 0:
                pl.semaphore_wait(barrier, n_dev - 1)
            for q in range(others):
                bias_copy(c, q).start()
        mt_ref[...] = m_ref[...].reshape(2 * m_ref.shape[1], n_res).astype(F32).T
        for c in range(chunks):
            for q in range(1, others):
                bias_copy(c, q).wait_recv()
                bias_forward(c, q).start()
        for k in range(1, n_dev):
            mask_copy(k).start()
        mask_own().start()
        for c in range(chunks):
            bias_copy(c, 0).wait_recv()
            for q in range(1, others):
                bias_forward(c, q).wait_recv()

        def turn(h, carry):
            bias_ref[h] = bias_all[h].astype(F32).T * LOG2E
            return carry

        lax.fori_loop(0, n_heads, turn, 0)
        for c in range(chunks):
            for q in range(others):
                bias_copy(c, q).wait_send()
            for q in range(1, others):
                bias_forward(c, q).wait_send()

    def load(u):
        row = pl.ds(t * pairs + u // 2, 1)
        return lambda: (e_ref[u % 2, u // 2], m_ref[u % 2, row, :].astype(F32))

    done = {}

    def emit(u, e1):
        done[u] = e1.astype(F32)
        if u % 2:
            turned[pl.ds(u // 2, n_res, stride=pairs), :] = jnp.concatenate([done.pop(u - 1), done.pop(u)], axis=0).T

    row_stream([load(u) for u in range(2 * pairs)], transposed(w_in_ref[...]), transposed(w_out_ref[...]), bias_ref, n_heads,
               n_res, emit)

    @pl.when(t >= 2)
    def _():
        for k in range(1, n_dev):
            tile_copy(t - 2, k).wait_send()
        tile_own(t - 2).wait()

    outbox[lax.rem(t, 2)] = turned[...].reshape(n_res, pairs, chans).astype(BF)
    for k in range(1, n_dev):
        tile_copy(t, k).start()
    tile_own(t).start()

    @pl.when(t == n_tiles - 1)
    def _():
        for tile in range(max(static_tiles - 2, 0), static_tiles):
            for k in range(1, n_dev):
                tile_copy(tile, k).wait_send()
            tile_own(tile).wait()
        for k in range(1, n_dev):
            mask_copy(k).wait_send()
            mask_copy(k).wait_recv()
        mask_own().wait()
        for tile in range(static_tiles):
            for k in range(1, n_dev):
                tile_copy(tile, k).wait_recv()


def row_attention(n_dev, e_t, mask, pair, w_pair_t, w_in, w_out):
    n_seq, chans, n_res = e_t.shape
    half = n_seq // 2
    tiles = half // TILE_PAIRS
    share = n_res // n_dev
    n_heads = w_pair_t.shape[0]
    e_t = e_t.reshape(2, half, chans, n_res)
    mask = mask.reshape(2, half, n_res)

    def whole(a):
        return pl.BlockSpec(a.shape, lambda t: (0,) * a.ndim)

    return pl.pallas_call(
        functools.partial(row_kernel, n_dev),
        grid=(tiles,),
        in_specs=[
            pl.BlockSpec((2, TILE_PAIRS, chans, n_res), lambda t: (0, t, 0, 0)),
            whole(mask), pl.BlockSpec(memory_space=pl.ANY), whole(w_pair_t), whole(w_in), whole(w_out),
        ],
        out_specs=[pl.BlockSpec(memory_space=pl.ANY), pl.BlockSpec(memory_space=pl.ANY)],
        out_shape=[
            jax.ShapeDtypeStruct((n_dev, share, half, 2 * chans), BF),
            jax.ShapeDtypeStruct((share, n_dev * n_seq), F32),
        ],
        scratch_shapes=[
            pltpu.VMEM((n_res * TILE_PAIRS, 2 * chans), F32),
            pltpu.VMEM((2, n_res, TILE_PAIRS, 2 * chans), BF),
            pltpu.VMEM(pair.shape, BF),
            pltpu.VMEM((n_res, n_seq), F32),
            pltpu.VMEM((n_res // 128, n_heads * share, 128), F32),
            pltpu.VMEM((n_heads, n_res, n_res), BF),
            pltpu.VMEM((n_heads, n_res, n_res), F32),
            pltpu.SemaphoreType.DMA((2, n_dev)),
            pltpu.SemaphoreType.DMA((tiles, n_dev)),
            pltpu.SemaphoreType.DMA((2,)),
            pltpu.SemaphoreType.DMA((n_dev,)),
            pltpu.SemaphoreType.DMA((n_dev,)),
            pltpu.SemaphoreType.DMA,
            pltpu.SemaphoreType.DMA((share // BIAS_ROWS,)),
        ] + [pltpu.SemaphoreType.DMA((share // BIAS_ROWS, n_dev // 2))] * 4,
        compiler_params=pltpu.CompilerParams(
            dimension_semantics=('arbitrary',), vmem_limit_bytes=VMEM_BYTES, collective_id=0, has_side_effects=True),
        name='row_attention',
    )(e_t, mask, pair, w_pair_t, w_in, w_out)


def col_kernel(n_heads, r_ref, m_ref, wc_ref, wco_ref, wti_ref, wto_ref, o_ref):
    n_dev, n_i, half, lanes = r_ref.shape
    chans = lanes // 2
    width = wco_ref.shape[0]
    d = width // n_heads
    eye = jnp.where(lax.broadcasted_iota(jnp.int32, (lanes, lanes), 0) == lax.broadcasted_iota(jnp.int32, (lanes, lanes), 1),
                    1.0, 0.0).astype(BF)
    low = lax.broadcasted_iota(jnp.int32, (chans, 2 * half), 1) < half
    same_head = (lax.broadcasted_iota(jnp.int32, (width, width), 0) // d
                 == lax.broadcasted_iota(jnp.int32, (width, width), 1) // d)
    w_t = wc_ref[...].astype(F32).T
    wc = jnp.concatenate([w_t[:width]] + [w_t[width:width + d]] * n_heads + [w_t[width + d:width + 2 * d]] * n_heads
                         + [w_t[width + 2 * d:]], axis=0).astype(BF)
    wco, wti, wto = transposed(wco_ref[...]), transposed(wti_ref[...]), wto_ref[...]
    state = [dict() for _ in range(n_i)]

    def turn(i):
        state[i]['turned'] = dot_nt(eye, r_ref[:, i].reshape(n_dev * half, lanes))

    def project(i):
        s = state[i]
        turned = s.pop('turned')
        cols = []
        for n in range(n_dev // 2):
            a = turned[:chans, n * 2 * half:(n + 1) * 2 * half]
            b = turned[chans:, n * 2 * half:(n + 1) * 2 * half]
            cols.append(jnp.where(low, a, pltpu.roll(b, half, 1)))
            cols.append(jnp.where(low, pltpu.roll(a, half, 1), b))
        s['x'] = jnp.concatenate(cols, axis=1)
        s['proj'] = dot(wc, norm_rows(s['x'])).astype(BF)

    def q_mean(i):
        s = state[i]
        m = m_ref[pl.ds(i, 1), :]
        q_sum = jnp.sum(s['proj'][:width].astype(F32) * m, axis=1, keepdims=True)
        count = jnp.sum(m, axis=1, keepdims=True)
        mean = jnp.broadcast_to(q_sum / (count + MEAN_EPS), (width, width))
        s['q_rows'] = jnp.where(same_head, mean.T, 0.0).astype(BF)

    def logits(i):
        s = state[i]
        s['logits'] = dot(s.pop('q_rows'), s['proj'][width:2 * width])

    def softmax(i):
        s = state[i]
        proj = s.pop('proj')
        t = s.pop('logits') * (d ** -0.5) + MASK_BIG * (m_ref[pl.ds(i, 1), :] - 1.0)
        e = jnp.exp(t - jnp.max(t, axis=1, keepdims=True))
        den = jnp.sum(e, axis=1, keepdims=True)
        num = jnp.sum(e * proj[2 * width:3 * width].astype(F32), axis=1, keepdims=True)
        s['gated'] = (jax.nn.sigmoid(proj[3 * width:].astype(F32)) * (num / den)).astype(BF)

    def out(i):
        s = state[i]
        s['e2'] = (s.pop('x') + dot(wco, s.pop('gated'))).astype(BF)

    def hidden(i):
        s = state[i]
        s['hidden'] = jnp.maximum(dot(wti, norm_rows(s['e2'].astype(F32))), 0.0).astype(BF)

    def finish(i):
        s = state[i]
        o_ref[i] = (s.pop('e2').astype(F32) + dot(wto, s.pop('hidden'))).astype(BF)

    stages = dict(turn=turn, project=project, q_mean=q_mean, logits=logits, softmax=softmax, out=out, hidden=hidden, finish=finish)
    for step in range(n_i + max(lag for _, lag in COL_STAGES)):
        for name, lag in COL_STAGES:
            if 0 <= step - lag < n_i:
                stages[name](step - lag)


def column_and_transition(n_heads, received, mask, wc, wco, wti, wto):
    n_dev, share, half, lanes = received.shape
    n_seq = mask.shape[1]

    def whole(a):
        return pl.BlockSpec(a.shape, lambda n: (0,) * a.ndim)

    return pl.pallas_call(
        functools.partial(col_kernel, n_heads),
        grid=(share // TILE_RES,),
        in_specs=[
            pl.BlockSpec((n_dev, TILE_RES, half, lanes), lambda n: (0, n, 0, 0)),
            pl.BlockSpec((TILE_RES, n_seq), lambda n: (n, 0)),
            whole(wc), whole(wco), whole(wti), whole(wto),
        ],
        out_specs=pl.BlockSpec((TILE_RES, lanes // 2, n_seq), lambda n: (n, 0, 0)),
        out_shape=jax.ShapeDtypeStruct((share, lanes // 2, n_seq), BF),
        compiler_params=pltpu.CompilerParams(dimension_semantics=('arbitrary',), vmem_limit_bytes=VMEM_BYTES),
        name='column_and_transition',
    )(received, mask, wc, wco, wti, wto)


def solution(mesh):
    n_dev = mesh.shape['seq']

    def local_block(msa, mask, pair, w_pair_bias, w_row_in, w_row_out, w_col_in, w_col_out, w_trans_in, w_trans_out):
        n_heads = w_pair_bias.shape[1]
        received, mask_cols = row_attention(
            n_dev, jnp.transpose(msa, (0, 2, 1)), mask, pair, w_pair_bias.T, w_row_in, w_row_out)
        out = column_and_transition(n_heads, received, mask_cols, w_col_in, w_col_out, w_trans_in, w_trans_out.T)
        return jnp.transpose(out, (2, 0, 1))

    rows = P(('batch', 'seq'))
    return jax.shard_map(local_block, mesh=mesh, in_specs=(rows, rows, rows) + (P(),) * 7, out_specs=P('batch', 'seq'),
                         check_vma=False)
```

```python
import functools

import jax
import jax.numpy as jnp
import numpy as np
from jax import lax
from jax.experimental import pallas as pl
from jax.experimental.pallas import tpu as pltpu
from jax.sharding import PartitionSpec as P

LN_EPS = 1.0e-5
MASK_BIG = 1.0e9
MEAN_EPS = 1.0e-10
LOG2E = 1.4426950408889634
BF = jnp.bfloat16
F32 = jnp.float32
MESH = pl.DeviceIdType.MESH

VMEM_BYTES = 67_043_328

TILE_PAIRS = 8
ROW_TIME = dict(norm=-6, project=-5, split=-3, logits=0, softmax=4, values=5, divide=8, gate=9, out=10, emit=11)
ROW_ORDER = ('logits', 'values', 'project', 'out', 'softmax', 'norm', 'split', 'divide', 'gate', 'emit')
TILE_RES = 16
COL_STAGES = (('finish', 5), ('hidden', 4), ('out', 3), ('logits', 2), ('project', 1), ('turn', 0), ('softmax', 2), ('q_mean', 1))
BIAS_ROWS = 16
FAR = 6


def norm_rows(x):
    n = x.shape[0]
    mean = jnp.sum(x, axis=0, keepdims=True) * (1.0 / n)
    centered = x - mean
    var = jnp.sum(centered * centered, axis=0, keepdims=True) * (1.0 / n)
    return (centered * lax.rsqrt(var + LN_EPS)).astype(BF)


def dot(a, b):
    return lax.dot_general(a, b, (((1,), (0,)), ((), ())), preferred_element_type=F32)


def dot_nt(a, b):
    return lax.dot_general(a, b, (((1,), (1,)), ((), ())), preferred_element_type=F32)


def split_bf16(value, parts):
    out, rest = [], np.float64(value)
    for _ in range(parts):
        part = np.float64(np.asarray(rest, np.float32).astype(np.dtype(BF)))
        out.append(float(part))
        rest = rest - part
    return out


def transposed(w):
    return w.astype(F32).T.astype(BF)


class Prologue:
    def __init__(self, w_in_t, width, head_dim):
        self.w_in_t, self.width, self.head_dim = w_in_t, width, head_dim

    def norm(self, s, x_bf, m_row):
        x = x_bf.astype(F32)
        s.update(x=x, m_row=m_row, y=norm_rows(x))

    def project(self, s):
        s['proj'] = dot(self.w_in_t, s.pop('y')).astype(BF)

    def split(self, s):
        width = self.width
        proj = s.pop('proj')
        q = proj[:width].astype(F32) * (self.head_dim ** -0.5 * LOG2E)
        q_hi = q.astype(BF)
        k = proj[width:2 * width]
        m_rows = jnp.broadcast_to(s.pop('m_row') - 1.0, (16, proj.shape[1])).astype(BF)
        s.update(q_hi=q_hi, q_lo=(q - q_hi.astype(F32)).astype(BF), v=proj[2 * width:3 * width], g=proj[3 * width:],
                 keys=jnp.concatenate([k, k, m_rows], axis=0).T)

    def save(self, s, kept_ref, keys_ref):
        kept_ref[...] = jnp.concatenate([s['q_hi'], s['q_lo'], s['v'], s['g']], axis=0)
        keys_ref[...] = s['keys']

    def restore(self, x_bf, kept_ref, keys_ref):
        q_hi, q_lo, v, g = (kept_ref[n * self.width:(n + 1) * self.width] for n in range(4))
        return dict(x=x_bf.astype(F32), q_hi=q_hi, q_lo=q_lo, v=v, g=g, keys=keys_ref[...])


def row_stream(loads, first, prologue, save_next, w_out_t, bias_ref, n_heads, n_res, emit):
    width = w_out_t.shape[1]
    d = width // n_heads
    row_id = lax.broadcasted_iota(jnp.int32, (16, n_res), 0)
    mask_rows = jnp.zeros((16, n_res), F32)
    for n, term in enumerate(split_bf16(MASK_BIG * LOG2E, 3)):
        mask_rows = jnp.where(row_id == n, term, mask_rows)
    mask_rows = mask_rows.astype(BF)
    per_tile = 16 // d
    zero = jnp.zeros((16, n_res), BF)
    ones = jnp.ones((8, n_res), F32)
    state = [first] + [dict() for _ in loads[1:]]

    def norm(i, h):
        prologue.norm(state[i], *loads[i]())

    def project(i, h):
        prologue.project(state[i])

    def split(i, h):
        prologue.split(state[i])
        if i == len(loads) - 1:
            save_next(state[i])

    def only_head(q, h):
        mine = h // per_tile
        own = jnp.where(row_id // d == h % per_tile, q[mine * 16:(mine + 1) * 16], zero)
        return [own if n == mine else zero for n in range(width // 16)]

    def logits(i, h):
        s = state[i]
        rhs = jnp.concatenate(only_head(s['q_hi'], h) + only_head(s['q_lo'], h) + [mask_rows], axis=0)
        s['t', h] = dot(s['keys'], rhs) + bias_ref[h]

    def softmax(i, h):
        t = state[i].pop(('t', h))
        state[i]['p', h] = jnp.exp2(t - jnp.max(t, axis=0, keepdims=True)).astype(BF)

    def values(i, h):
        s = state[i]
        lhs = jnp.concatenate([s['v'][h * d:(h + 1) * d].astype(F32), ones], axis=0).astype(BF)
        s['o', h] = dot(lhs, s.pop(('p', h)))

    def divide(i, h):
        o = state[i].pop(('o', h))
        state[i]['r', h] = o[:d] / o[d:d + 8]

    def gate(i, h):
        s = state[i]
        o = jnp.concatenate([s.pop(('r', n)) for n in range(n_heads)], axis=0)
        s['gated'] = (jax.nn.sigmoid(s.pop('g').astype(F32)) * o).astype(BF)

    def out(i, h):
        state[i]['u'] = dot(w_out_t, state[i].pop('gated'))

    def last(i, h):
        s = state[i]
        emit(i, (s.pop('x') + s.pop('u')).astype(BF))
        s.clear()

    stages = dict(norm=norm, project=project, split=split, logits=logits, softmax=softmax, values=values, divide=divide,
                  gate=gate, out=out, emit=last)
    first_stages, end = ('norm', 'project', 'split'), ('gate', 'out', 'emit')
    events = []
    for i in range(len(loads)):
        for rank, name in enumerate(ROW_ORDER):
            if (i == 0 and name in first_stages) or (i == len(loads) - 1 and name not in first_stages):
                continue
            heads = [0] if name in first_stages else [n_heads - 1] if name in end else range(n_heads)
            events += [(n_heads * i + h + ROW_TIME[name], rank, i, h, name) for h in heads]
    for _, _, i, h, name in sorted(events):
        stages[name](i, h)


def row_kernel(n_dev, e_ref, e_next_ref, m_ref, z_hbm, w_pair_ref, w_in_ref, w_out_ref, recv_ref, mrecv_ref,
               turned, outbox, z_ref, mt_ref, bias_rows, bias_all, bias_ref, kept_ref, keys_ref, relay, relay_sem, on_sem, send_sem, recv_sem, own_sem, msend_sem, mrecv_sem,
               mown_sem, z_sem, bsend_sem, brecv_sem, fsend_sem, frecv_sem):
    t = pl.program_id(0)
    n_tiles = pl.num_programs(0)
    static_tiles = recv_sem.shape[0]
    me = lax.axis_index('seq')
    n_heads, _, n_res = bias_ref.shape
    pairs = e_ref.shape[1]
    share = n_res // n_dev
    n_local = mt_ref.shape[1]
    chans = turned.shape[1]

    def wrap(i):
        return lax.rem(i + n_dev, n_dev)

    def mate(i):
        return i + 1 - 2 * lax.rem(i, 2)

    ahead_chip, behind_chip, far_chip = wrap(me + 2), wrap(me - 2), wrap(me + n_dev // 2)
    peers = [me, mate(me), ahead_chip, mate(ahead_chip), behind_chip, mate(behind_chip), far_chip, mate(far_chip)]

    def peer(k):
        return peers[k]

    def mask_copy(k):
        d = peer(k)
        return pltpu.make_async_remote_copy(
            src_ref=mt_ref.at[pl.ds(pl.multiple_of(d * share, share), share)],
            dst_ref=mrecv_ref.at[:, pl.ds(pl.multiple_of(me * n_local, n_local), n_local)],
            send_sem=msend_sem.at[k], recv_sem=mrecv_sem.at[k], device_id={'seq': d}, device_id_type=MESH)

    def mask_own():
        return pltpu.make_async_copy(
            mt_ref.at[pl.ds(pl.multiple_of(me * share, share), share)],
            mrecv_ref.at[:, pl.ds(pl.multiple_of(me * n_local, n_local), n_local)], mown_sem)

    def tile_copy(tile, k):
        d = peer(k)
        slot = lax.rem(tile, 2)
        return pltpu.make_async_remote_copy(
            src_ref=outbox.at[slot, pl.ds(d * share, share)],
            dst_ref=recv_ref.at[me, :, pl.ds(pl.multiple_of(tile * pairs, pairs), pairs), :],
            send_sem=send_sem.at[slot, k], recv_sem=recv_sem.at[tile, k], device_id={'seq': d}, device_id_type=MESH)

    def relay_out(tile, r):
        slot = lax.rem(tile, 2)
        return pltpu.make_async_remote_copy(
            src_ref=outbox.at[slot, pl.ds(peer(FAR + r) * share, share)], dst_ref=relay.at[tile, r],
            send_sem=send_sem.at[slot, FAR + r], recv_sem=relay_sem.at[tile, r],
            device_id={'seq': (ahead_chip, behind_chip)[r]}, device_id_type=MESH)

    def relay_on(tile, r):
        owner = (behind_chip, ahead_chip)[r]
        to = (ahead_chip, mate(behind_chip))[r]
        return pltpu.make_async_remote_copy(
            src_ref=relay.at[tile, r],
            dst_ref=recv_ref.at[owner, :, pl.ds(pl.multiple_of(tile * pairs, pairs), pairs), :],
            send_sem=on_sem.at[tile, r], recv_sem=recv_sem.at[tile, FAR + r], device_id={'seq': to}, device_id_type=MESH)

    def wait_sent(tile):
        for k in range(1, FAR):
            tile_copy(tile, k).wait_send()
        for r in range(2):
            relay_out(tile, r).wait_send()
        tile_own(tile).wait()

    def pass_on(tile):
        for r in range(2):
            relay_out(tile, r).wait_recv()
            relay_on(tile, r).start()

    def tile_own(tile):
        slot = lax.rem(tile, 2)
        return pltpu.make_async_copy(
            outbox.at[slot, pl.ds(me * share, share)],
            recv_ref.at[me, :, pl.ds(pl.multiple_of(tile * pairs, pairs), pairs), :], own_sem.at[slot])

    chunks = share // BIAS_ROWS
    others = n_dev // 2
    partner = me + 1 - 2 * lax.rem(me, 2)

    def bias_block(owner, c):
        return bias_all.at[:, pl.ds(pl.multiple_of(owner * share + c * BIAS_ROWS, BIAS_ROWS), BIAS_ROWS), :]

    def bias_copy(c, q):
        to = partner if q == 0 else lax.rem(me + 2 * q, n_dev)
        return pltpu.make_async_remote_copy(
            src_ref=bias_block(me, c), dst_ref=bias_block(me, c), send_sem=bsend_sem.at[c, q], recv_sem=brecv_sem.at[c, q],
            device_id={'seq': to}, device_id_type=MESH)

    def bias_forward(c, q):
        owner = lax.rem(me + n_dev - 2 * q, n_dev)
        return pltpu.make_async_remote_copy(
            src_ref=bias_block(owner, c), dst_ref=bias_block(owner, c), send_sem=fsend_sem.at[c, q],
            recv_sem=frecv_sem.at[c, q], device_id={'seq': partner}, device_id_type=MESH)

    def z_copy(c):
        rows = pl.ds(c * BIAS_ROWS, BIAS_ROWS)
        return pltpu.make_async_copy(z_hbm.at[rows], z_ref.at[rows], z_sem.at[c])

    width = w_out_ref.shape[0]
    prologue = Prologue(transposed(w_in_ref[...]), width, width // n_heads)

    def mask_row(half, row):
        return m_ref[half, pl.ds(row, 1), :].astype(F32)

    @pl.when(t == 0)
    def _():
        for c in range(chunks):
            z_copy(c).start()
        barrier = pltpu.get_barrier_semaphore()
        for k in range(1, n_dev):
            pl.semaphore_signal(barrier, inc=1, device_id={'seq': peer(k)}, device_id_type=MESH)
        z_ch = z_ref.shape[2]
        eye = jnp.where(lax.broadcasted_iota(jnp.int32, (z_ch, z_ch), 0) == lax.broadcasted_iota(jnp.int32, (z_ch, z_ch), 1),
                        1.0, 0.0).astype(BF)
        w_pair = w_pair_ref[...]
        for c in range(chunks):
            z_copy(c).wait()

            at = [c * BIAS_ROWS + n for n in range(0, BIAS_ROWS, 4)]
            turned_z = [dot_nt(eye, z_ref[i:i + 4].reshape(4 * n_res, z_ch)) for i in at]
            normed = [norm_rows(z) for z in turned_z]
            b = [dot(w_pair, z) for z in normed]
            for n, i in enumerate(at):
                for u in range(4):
                    for part in range(n_res // 128):
                        lane = u * n_res + part * 128
                        bias_rows[part, pl.ds(i + u, n_heads, stride=share), :] = b[n][:, lane:lane + 128]
            for part in range(n_res // 128):
                own = bias_rows[part].reshape(n_heads, share, 128)[:, c * BIAS_ROWS:(c + 1) * BIAS_ROWS]
                bias_all[:, pl.ds(pl.multiple_of(me * share + c * BIAS_ROWS, BIAS_ROWS), BIAS_ROWS),
                         part * 128:(part + 1) * 128] = own.astype(BF)
            if c == 0:
                pl.semaphore_wait(barrier, n_dev - 1)
            for q in range(others):
                bias_copy(c, q).start()
        ahead = {}
        prologue.norm(ahead, e_ref[0, 0], mask_row(0, 0))
        prologue.project(ahead)
        prologue.split(ahead)
        prologue.save(ahead, kept_ref, keys_ref)
        mt_ref[...] = m_ref[...].reshape(2 * m_ref.shape[1], n_res).astype(F32).T
        for c in range(chunks):
            for q in range(1, others):
                bias_copy(c, q).wait_recv()
                bias_forward(c, q).start()
        for k in range(1, n_dev):
            mask_copy(k).start()
        mask_own().start()
        for c in range(chunks):
            bias_copy(c, 0).wait_recv()
            for q in range(1, others):
                bias_forward(c, q).wait_recv()

        for h in range(n_heads):
            bias_ref[h] = bias_all[h].astype(F32).T * LOG2E
        for c in range(chunks):
            for q in range(others):
                bias_copy(c, q).wait_send()
            for q in range(1, others):
                bias_forward(c, q).wait_send()

    def load(u):
        return lambda: (e_ref[u % 2, u // 2], mask_row(u % 2, t * pairs + u // 2))

    def load_next():
        return e_next_ref[0, 0], mask_row(0, lax.rem(t + 1, static_tiles) * pairs)

    done = {}

    def emit(u, e1):
        done[u] = e1.astype(F32)
        if u % 2:
            turned[pl.ds(u // 2, n_res, stride=pairs), :] = jnp.concatenate([done.pop(u - 1), done.pop(u)], axis=0).T

    row_stream([load(u) for u in range(2 * pairs)] + [load_next], prologue.restore(e_ref[0, 0], kept_ref, keys_ref), prologue,
               lambda s: prologue.save(s, kept_ref, keys_ref), transposed(w_out_ref[...]), bias_ref, n_heads, n_res, emit)

    @pl.when(t >= 2)
    def _():
        wait_sent(t - 2)

    outbox[lax.rem(t, 2)] = turned[...].reshape(n_res, pairs, chans).astype(BF)
    for r in range(2):
        relay_out(t, r).start()
    for k in (2, 4, 3, 5, 1):
        tile_copy(t, k).start()
    tile_own(t).start()

    @pl.when(t >= 1)
    def _():
        pass_on(t - 1)

    @pl.when(t == n_tiles - 1)
    def _():
        pass_on(static_tiles - 1)
        for tile in range(max(static_tiles - 2, 0), static_tiles):
            wait_sent(tile)
        for k in range(1, n_dev):
            mask_copy(k).wait_send()
            mask_copy(k).wait_recv()
        mask_own().wait()
        for tile in range(static_tiles):
            for r in range(2):
                relay_on(tile, r).wait_send()
            for k in range(1, n_dev):
                tile_copy(tile, k).wait_recv()


def row_attention(n_dev, e_t, mask, pair, w_pair_t, w_in, w_out):
    n_seq, chans, n_res = e_t.shape
    half = n_seq // 2
    tiles = half // TILE_PAIRS
    share = n_res // n_dev
    n_heads = w_pair_t.shape[0]
    width = w_out.shape[0]
    e_t = e_t.reshape(2, half, chans, n_res)
    mask = mask.reshape(2, half, n_res)

    def whole(a):
        return pl.BlockSpec(a.shape, lambda t: (0,) * a.ndim)

    return pl.pallas_call(
        functools.partial(row_kernel, n_dev),
        grid=(tiles,),
        in_specs=[
            pl.BlockSpec((2, TILE_PAIRS, chans, n_res), lambda t: (0, t, 0, 0)),
            pl.BlockSpec((1, 1, chans, n_res), lambda t: (0, lax.rem(t + 1, tiles) * TILE_PAIRS, 0, 0)),
            whole(mask), pl.BlockSpec(memory_space=pl.ANY), whole(w_pair_t), whole(w_in), whole(w_out),
        ],
        out_specs=[pl.BlockSpec(memory_space=pl.ANY), pl.BlockSpec(memory_space=pl.ANY)],
        out_shape=[
            jax.ShapeDtypeStruct((n_dev, share, half, 2 * chans), BF),
            jax.ShapeDtypeStruct((share, n_dev * n_seq), F32),
        ],
        scratch_shapes=[
            pltpu.VMEM((n_res * TILE_PAIRS, 2 * chans), F32),
            pltpu.VMEM((2, n_res, TILE_PAIRS, 2 * chans), BF),
            pltpu.VMEM(pair.shape, BF),
            pltpu.VMEM((n_res, n_seq), F32),
            pltpu.VMEM((n_res // 128, n_heads * share, 128), F32),
            pltpu.VMEM((n_heads, n_res, n_res), BF),
            pltpu.VMEM((n_heads, n_res, n_res), F32),
            pltpu.VMEM((4 * width, n_res), BF),
            pltpu.VMEM((n_res, 2 * width + 16), BF),
            pltpu.VMEM((tiles, 2, share, TILE_PAIRS, 2 * chans), BF),
            pltpu.SemaphoreType.DMA((tiles, 2)),
            pltpu.SemaphoreType.DMA((tiles, 2)),
            pltpu.SemaphoreType.DMA((2, n_dev)),
            pltpu.SemaphoreType.DMA((tiles, n_dev)),
            pltpu.SemaphoreType.DMA((2,)),
            pltpu.SemaphoreType.DMA((n_dev,)),
            pltpu.SemaphoreType.DMA((n_dev,)),
            pltpu.SemaphoreType.DMA,
            pltpu.SemaphoreType.DMA((share // BIAS_ROWS,)),
        ] + [pltpu.SemaphoreType.DMA((share // BIAS_ROWS, n_dev // 2))] * 4,
        compiler_params=pltpu.CompilerParams(
            dimension_semantics=('arbitrary',), vmem_limit_bytes=VMEM_BYTES, collective_id=0, has_side_effects=True),
        name='row_attention',
    )(e_t, e_t, mask, pair, w_pair_t, w_in, w_out)


def col_kernel(n_heads, r_ref, m_ref, wc_ref, wco_ref, wti_ref, wto_ref, o_ref):
    n_dev, n_i, half, lanes = r_ref.shape
    chans = lanes // 2
    width = wco_ref.shape[0]
    d = width // n_heads
    eye = jnp.where(lax.broadcasted_iota(jnp.int32, (lanes, lanes), 0) == lax.broadcasted_iota(jnp.int32, (lanes, lanes), 1),
                    1.0, 0.0).astype(BF)
    low = lax.broadcasted_iota(jnp.int32, (chans, 2 * half), 1) < half
    same_head = (lax.broadcasted_iota(jnp.int32, (width, width), 0) // d
                 == lax.broadcasted_iota(jnp.int32, (width, width), 1) // d)
    w_t = wc_ref[...].astype(F32).T
    wc = jnp.concatenate([w_t[:width]] + [w_t[width:width + d]] * n_heads + [w_t[width + d:width + 2 * d]] * n_heads
                         + [w_t[width + 2 * d:]], axis=0).astype(BF)
    wco, wti, wto = transposed(wco_ref[...]), transposed(wti_ref[...]), wto_ref[...]
    state = [dict() for _ in range(n_i)]

    def turn(i):
        state[i]['turned'] = dot_nt(eye, r_ref[:, i].reshape(n_dev * half, lanes))

    def project(i):
        s = state[i]
        turned = s.pop('turned')
        cols = []
        for n in range(n_dev // 2):
            a = turned[:chans, n * 2 * half:(n + 1) * 2 * half]
            b = turned[chans:, n * 2 * half:(n + 1) * 2 * half]
            cols.append(jnp.where(low, a, pltpu.roll(b, half, 1)))
            cols.append(jnp.where(low, pltpu.roll(a, half, 1), b))
        s['x'] = jnp.concatenate(cols, axis=1)
        s['proj'] = dot(wc, norm_rows(s['x'])).astype(BF)

    def q_mean(i):
        s = state[i]
        m = m_ref[pl.ds(i, 1), :]
        q_sum = jnp.sum(s['proj'][:width].astype(F32) * m, axis=1, keepdims=True)
        count = jnp.sum(m, axis=1, keepdims=True)
        mean = jnp.broadcast_to(q_sum / (count + MEAN_EPS), (width, width))
        s['q_rows'] = jnp.where(same_head, mean.T, 0.0).astype(BF)

    def logits(i):
        s = state[i]
        s['logits'] = dot(s.pop('q_rows'), s['proj'][width:2 * width])

    def softmax(i):
        s = state[i]
        proj = s.pop('proj')
        t = s.pop('logits') * (d ** -0.5) + MASK_BIG * (m_ref[pl.ds(i, 1), :] - 1.0)
        e = jnp.exp(t - jnp.max(t, axis=1, keepdims=True))
        den = jnp.sum(e, axis=1, keepdims=True)
        num = jnp.sum(e * proj[2 * width:3 * width].astype(F32), axis=1, keepdims=True)
        s['gated'] = (jax.nn.sigmoid(proj[3 * width:].astype(F32)) * (num / den)).astype(BF)

    def out(i):
        s = state[i]
        s['e2'] = (s.pop('x') + dot(wco, s.pop('gated'))).astype(BF)

    def hidden(i):
        s = state[i]
        s['hidden'] = jnp.maximum(dot(wti, norm_rows(s['e2'].astype(F32))), 0.0).astype(BF)

    def finish(i):
        s = state[i]
        o_ref[i] = (s.pop('e2').astype(F32) + dot(wto, s.pop('hidden'))).astype(BF)

    stages = dict(turn=turn, project=project, q_mean=q_mean, logits=logits, softmax=softmax, out=out, hidden=hidden, finish=finish)
    for step in range(n_i + max(lag for _, lag in COL_STAGES)):
        for name, lag in COL_STAGES:
            if 0 <= step - lag < n_i:
                stages[name](step - lag)


def column_and_transition(n_heads, received, mask, wc, wco, wti, wto):
    n_dev, share, half, lanes = received.shape
    n_seq = mask.shape[1]

    def whole(a):
        return pl.BlockSpec(a.shape, lambda n: (0,) * a.ndim)

    return pl.pallas_call(
        functools.partial(col_kernel, n_heads),
        grid=(share // TILE_RES,),
        in_specs=[
            pl.BlockSpec((n_dev, TILE_RES, half, lanes), lambda n: (0, n, 0, 0)),
            pl.BlockSpec((TILE_RES, n_seq), lambda n: (n, 0)),
            whole(wc), whole(wco), whole(wti), whole(wto),
        ],
        out_specs=pl.BlockSpec((TILE_RES, lanes // 2, n_seq), lambda n: (n, 0, 0)),
        out_shape=jax.ShapeDtypeStruct((share, lanes // 2, n_seq), BF),
        compiler_params=pltpu.CompilerParams(dimension_semantics=('arbitrary',), vmem_limit_bytes=VMEM_BYTES),
        name='column_and_transition',
    )(received, mask, wc, wco, wti, wto)


def solution(mesh):
    n_dev = mesh.shape['seq']

    def local_block(msa, mask, pair, w_pair_bias, w_row_in, w_row_out, w_col_in, w_col_out, w_trans_in, w_trans_out):
        n_heads = w_pair_bias.shape[1]
        received, mask_cols = row_attention(
            n_dev, jnp.transpose(msa, (0, 2, 1)), mask, pair, w_pair_bias.T, w_row_in, w_row_out)
        out = column_and_transition(n_heads, received, mask_cols, w_col_in, w_col_out, w_trans_in, w_trans_out.T)
        return jnp.transpose(out, (2, 0, 1))

    rows = P(('batch', 'seq'))
    return jax.shard_map(local_block, mesh=mesh, in_specs=(rows, rows, rows) + (P(),) * 7, out_specs=P('batch', 'seq'),
                         check_vma=False)
```

```python
import functools

import jax
import jax.numpy as jnp
import numpy as np
from jax import lax
from jax.experimental import pallas as pl
from jax.experimental.pallas import tpu as pltpu
from jax.sharding import PartitionSpec as P

LN_EPS = 1.0e-5
MASK_BIG = 1.0e9
MEAN_EPS = 1.0e-10
LOG2E = 1.4426950408889634
BF = jnp.bfloat16
F32 = jnp.float32
MESH = pl.DeviceIdType.MESH

VMEM_BYTES = 67_043_328

TILE_PAIRS = 8
ROW_TIME = dict(norm=-6, project=-5, split=-3, logits=0, softmax=4, values=5, divide=8, gate=9, out=10, emit=11)
ROW_ORDER = ('logits', 'values', 'project', 'out', 'softmax', 'norm', 'split', 'divide', 'gate', 'emit')
TILE_RES = 16
COL_STAGES = (('finish', 5), ('hidden', 4), ('out', 3), ('logits', 2), ('project', 1), ('turn', 0), ('softmax', 2), ('q_mean', 1))
BIAS_ROWS = 16


def norm_rows(x):
    n = x.shape[0]
    mean = jnp.sum(x, axis=0, keepdims=True) * (1.0 / n)
    centered = x - mean
    var = jnp.sum(centered * centered, axis=0, keepdims=True) * (1.0 / n)
    return (centered * lax.rsqrt(var + LN_EPS)).astype(BF)


def dot(a, b):
    return lax.dot_general(a, b, (((1,), (0,)), ((), ())), preferred_element_type=F32)


def dot_nt(a, b):
    return lax.dot_general(a, b, (((1,), (1,)), ((), ())), preferred_element_type=F32)


def split_bf16(value, parts):
    out, rest = [], np.float64(value)
    for _ in range(parts):
        part = np.float64(np.asarray(rest, np.float32).astype(np.dtype(BF)))
        out.append(float(part))
        rest = rest - part
    return out


def transposed(w):
    return w.astype(F32).T.astype(BF)


def row_stream(loads, w_in_t, w_out_t, bias_ref, n_heads, n_res, emit):
    width = w_out_t.shape[1]
    d = width // n_heads
    row_id = lax.broadcasted_iota(jnp.int32, (16, n_res), 0)
    mask_rows = jnp.zeros((16, n_res), F32)
    for n, term in enumerate(split_bf16(MASK_BIG * LOG2E, 3)):
        mask_rows = jnp.where(row_id == n, term, mask_rows)
    mask_rows = mask_rows.astype(BF)
    per_tile = 16 // d
    zero = jnp.zeros((16, n_res), BF)
    ones = jnp.ones((8, n_res), F32)
    state = [dict() for _ in loads]

    def norm(i, h):
        x_bf, m_row = loads[i]()
        x = x_bf.astype(F32)
        state[i].update(x=x, m_row=m_row, y=norm_rows(x))

    def project(i, h):
        state[i]['proj'] = dot(w_in_t, state[i].pop('y')).astype(BF)

    def split(i, h):
        s = state[i]
        proj = s.pop('proj')
        q = proj[:width].astype(F32) * (d ** -0.5 * LOG2E)
        q_hi = q.astype(BF)
        k = proj[width:2 * width]
        m_rows = jnp.broadcast_to(s.pop('m_row') - 1.0, (16, n_res)).astype(BF)
        s.update(q_hi=q_hi, q_lo=(q - q_hi.astype(F32)).astype(BF), v=proj[2 * width:3 * width], g=proj[3 * width:],
                 keys=jnp.concatenate([k, k, m_rows], axis=0).T)

    def only_head(q, h):
        mine = h // per_tile
        own = jnp.where(row_id // d == h % per_tile, q[mine * 16:(mine + 1) * 16], zero)
        return [own if n == mine else zero for n in range(width // 16)]

    def logits(i, h):
        s = state[i]
        rhs = jnp.concatenate(only_head(s['q_hi'], h) + only_head(s['q_lo'], h) + [mask_rows], axis=0)
        s['t', h] = dot(s['keys'], rhs) + bias_ref[h]

    def softmax(i, h):
        t = state[i].pop(('t', h))
        state[i]['p', h] = jnp.exp2(t - jnp.max(t, axis=0, keepdims=True)).astype(BF)

    def values(i, h):
        s = state[i]
        lhs = jnp.concatenate([s['v'][h * d:(h + 1) * d].astype(F32), ones], axis=0).astype(BF)
        s['o', h] = dot(lhs, s.pop(('p', h)))

    def divide(i, h):
        o = state[i].pop(('o', h))
        state[i]['r', h] = o[:d] / o[d:d + 8]

    def gate(i, h):
        s = state[i]
        o = jnp.concatenate([s.pop(('r', n)) for n in range(n_heads)], axis=0)
        s['gated'] = (jax.nn.sigmoid(s.pop('g').astype(F32)) * o).astype(BF)

    def out(i, h):
        state[i]['u'] = dot(w_out_t, state[i].pop('gated'))

    def last(i, h):
        s = state[i]
        emit(i, (s.pop('x') + s.pop('u')).astype(BF))
        s.clear()

    stages = dict(norm=norm, project=project, split=split, logits=logits, softmax=softmax, values=values, divide=divide,
                  gate=gate, out=out, emit=last)
    first, end = ('norm', 'project', 'split'), ('gate', 'out', 'emit')
    events = []
    for i in range(len(loads)):
        for rank, name in enumerate(ROW_ORDER):
            heads = [0] if name in first else [n_heads - 1] if name in end else range(n_heads)
            events += [(n_heads * i + h + ROW_TIME[name], rank, i, h, name) for h in heads]
    for _, _, i, h, name in sorted(events):
        stages[name](i, h)


def row_kernel(n_dev, e_ref, m_ref, z_hbm, w_pair_ref, w_in_ref, w_out_ref, recv_ref, mrecv_ref,
               turned, outbox, z_ref, mt_ref, bias_rows, bias_all, bias_ref, send_sem, recv_sem, own_sem, msend_sem, mrecv_sem,
               mown_sem, z_sem, bsend_sem, brecv_sem, fsend_sem, frecv_sem):
    t = pl.program_id(0)
    n_tiles = pl.num_programs(0)
    static_tiles = recv_sem.shape[0]
    me = lax.axis_index('seq')
    n_heads, _, n_res = bias_ref.shape
    pairs = e_ref.shape[1]
    share = n_res // n_dev
    n_local = mt_ref.shape[1]
    chans = turned.shape[1]

    def peer(k):
        return lax.rem(me + k, n_dev)

    def mask_copy(k):
        d = peer(k)
        return pltpu.make_async_remote_copy(
            src_ref=mt_ref.at[pl.ds(pl.multiple_of(d * share, share), share)],
            dst_ref=mrecv_ref.at[:, pl.ds(pl.multiple_of(me * n_local, n_local), n_local)],
            send_sem=msend_sem.at[k], recv_sem=mrecv_sem.at[k], device_id={'seq': d}, device_id_type=MESH)

    def mask_own():
        return pltpu.make_async_copy(
            mt_ref.at[pl.ds(pl.multiple_of(me * share, share), share)],
            mrecv_ref.at[:, pl.ds(pl.multiple_of(me * n_local, n_local), n_local)], mown_sem)

    def tile_copy(tile, k):
        d = peer(k)
        slot = lax.rem(tile, 2)
        return pltpu.make_async_remote_copy(
            src_ref=outbox.at[slot, pl.ds(d * share, share)],
            dst_ref=recv_ref.at[me, :, pl.ds(pl.multiple_of(tile * pairs, pairs), pairs), :],
            send_sem=send_sem.at[slot, k], recv_sem=recv_sem.at[tile, k], device_id={'seq': d}, device_id_type=MESH)

    def tile_own(tile):
        slot = lax.rem(tile, 2)
        return pltpu.make_async_copy(
            outbox.at[slot, pl.ds(me * share, share)],
            recv_ref.at[me, :, pl.ds(pl.multiple_of(tile * pairs, pairs), pairs), :], own_sem.at[slot])

    chunks = share // BIAS_ROWS
    others = n_dev // 2
    partner = me + 1 - 2 * lax.rem(me, 2)

    def bias_block(owner, c):
        return bias_all.at[:, pl.ds(pl.multiple_of(owner * share + c * BIAS_ROWS, BIAS_ROWS), BIAS_ROWS), :]

    def bias_copy(c, q):
        to = partner if q == 0 else lax.rem(me + 2 * q, n_dev)
        return pltpu.make_async_remote_copy(
            src_ref=bias_block(me, c), dst_ref=bias_block(me, c), send_sem=bsend_sem.at[c, q], recv_sem=brecv_sem.at[c, q],
            device_id={'seq': to}, device_id_type=MESH)

    def bias_forward(c, q):
        owner = lax.rem(me + n_dev - 2 * q, n_dev)
        return pltpu.make_async_remote_copy(
            src_ref=bias_block(owner, c), dst_ref=bias_block(owner, c), send_sem=fsend_sem.at[c, q],
            recv_sem=frecv_sem.at[c, q], device_id={'seq': partner}, device_id_type=MESH)

    def z_copy(c):
        rows = pl.ds(c * BIAS_ROWS, BIAS_ROWS)
        return pltpu.make_async_copy(z_hbm.at[rows], z_ref.at[rows], z_sem.at[c])

    @pl.when(t == 0)
    def _():
        for c in range(chunks):
            z_copy(c).start()
        barrier = pltpu.get_barrier_semaphore()
        for k in range(1, n_dev):
            pl.semaphore_signal(barrier, inc=1, device_id={'seq': peer(k)}, device_id_type=MESH)
        z_ch = z_ref.shape[2]
        eye = jnp.where(lax.broadcasted_iota(jnp.int32, (z_ch, z_ch), 0) == lax.broadcasted_iota(jnp.int32, (z_ch, z_ch), 1),
                        1.0, 0.0).astype(BF)
        w_pair = w_pair_ref[...]
        for c in range(chunks):
            z_copy(c).wait()

            def rows_step(n, carry, c=c):
                i = c * BIAS_ROWS + n * 4
                turned_z = dot_nt(eye, z_ref[pl.ds(i, 4)].reshape(4 * n_res, z_ch))
                b = dot(w_pair, norm_rows(turned_z))
                for u in range(4):
                    for part in range(n_res // 128):
                        at = u * n_res + part * 128
                        bias_rows[part, pl.ds(i + u, n_heads, stride=share), :] = b[:, at:at + 128]
                return carry

            lax.fori_loop(0, BIAS_ROWS // 4, rows_step, 0)
            for part in range(n_res // 128):
                own = bias_rows[part].reshape(n_heads, share, 128)[:, c * BIAS_ROWS:(c + 1) * BIAS_ROWS]
                bias_all[:, pl.ds(pl.multiple_of(me * share + c * BIAS_ROWS, BIAS_ROWS), BIAS_ROWS),
                         part * 128:(part + 1) * 128] = own.astype(BF)
            if c == 0:
                pl.semaphore_wait(barrier, n_dev - 1)
            for q in range(others):
                bias_copy(c, q).start()
        mt_ref[...] = m_ref[...].reshape(2 * m_ref.shape[1], n_res).astype(F32).T
        for c in range(chunks):
            for q in range(1, others):
                bias_copy(c, q).wait_recv()
                bias_forward(c, q).start()
        for k in range(1, n_dev):
            mask_copy(k).start()
        mask_own().start()
        for c in range(chunks):
            bias_copy(c, 0).wait_recv()
            for q in range(1, others):
                bias_forward(c, q).wait_recv()

        def turn(h, carry):
            bias_ref[h] = bias_all[h].astype(F32).T * LOG2E
            return carry

        lax.fori_loop(0, n_heads, turn, 0)
        for c in range(chunks):
            for q in range(others):
                bias_copy(c, q).wait_send()
            for q in range(1, others):
                bias_forward(c, q).wait_send()

    def load(u):
        row = pl.ds(t * pairs + u // 2, 1)
        return lambda: (e_ref[u % 2, u // 2], m_ref[u % 2, row, :].astype(F32))

    done = {}

    def emit(u, e1):
        done[u] = e1.astype(F32)
        if u % 2:
            turned[pl.ds(u // 2, n_res, stride=pairs), :] = jnp.concatenate([done.pop(u - 1), done.pop(u)], axis=0).T

    row_stream([load(u) for u in range(2 * pairs)], transposed(w_in_ref[...]), transposed(w_out_ref[...]), bias_ref, n_heads,
               n_res, emit)

    @pl.when(t >= 2)
    def _():
        for k in range(1, n_dev):
            tile_copy(t - 2, k).wait_send()
        tile_own(t - 2).wait()

    outbox[lax.rem(t, 2)] = turned[...].reshape(n_res, pairs, chans).astype(BF)
    for k in sorted(range(1, n_dev), key=lambda k: -min(k, n_dev - k)):
        tile_copy(t, k).start()
    tile_own(t).start()

    @pl.when(t == n_tiles - 1)
    def _():
        for tile in range(max(static_tiles - 2, 0), static_tiles):
            for k in range(1, n_dev):
                tile_copy(tile, k).wait_send()
            tile_own(tile).wait()
        for k in range(1, n_dev):
            mask_copy(k).wait_send()
            mask_copy(k).wait_recv()
        mask_own().wait()
        for tile in range(static_tiles):
            for k in range(1, n_dev):
                tile_copy(tile, k).wait_recv()


def row_attention(n_dev, e_t, mask, pair, w_pair_t, w_in, w_out):
    n_seq, chans, n_res = e_t.shape
    half = n_seq // 2
    tiles = half // TILE_PAIRS
    share = n_res // n_dev
    n_heads = w_pair_t.shape[0]
    e_t = e_t.reshape(2, half, chans, n_res)
    mask = mask.reshape(2, half, n_res)

    def whole(a):
        return pl.BlockSpec(a.shape, lambda t: (0,) * a.ndim)

    return pl.pallas_call(
        functools.partial(row_kernel, n_dev),
        grid=(tiles,),
        in_specs=[
            pl.BlockSpec((2, TILE_PAIRS, chans, n_res), lambda t: (0, t, 0, 0)),
            whole(mask), pl.BlockSpec(memory_space=pl.ANY), whole(w_pair_t), whole(w_in), whole(w_out),
        ],
        out_specs=[pl.BlockSpec(memory_space=pl.ANY), pl.BlockSpec(memory_space=pl.ANY)],
        out_shape=[
            jax.ShapeDtypeStruct((n_dev, share, half, 2 * chans), BF),
            jax.ShapeDtypeStruct((share, n_dev * n_seq), F32),
        ],
        scratch_shapes=[
            pltpu.VMEM((n_res * TILE_PAIRS, 2 * chans), F32),
            pltpu.VMEM((2, n_res, TILE_PAIRS, 2 * chans), BF),
            pltpu.VMEM(pair.shape, BF),
            pltpu.VMEM((n_res, n_seq), F32),
            pltpu.VMEM((n_res // 128, n_heads * share, 128), F32),
            pltpu.VMEM((n_heads, n_res, n_res), BF),
            pltpu.VMEM((n_heads, n_res, n_res), F32),
            pltpu.SemaphoreType.DMA((2, n_dev)),
            pltpu.SemaphoreType.DMA((tiles, n_dev)),
            pltpu.SemaphoreType.DMA((2,)),
            pltpu.SemaphoreType.DMA((n_dev,)),
            pltpu.SemaphoreType.DMA((n_dev,)),
            pltpu.SemaphoreType.DMA,
            pltpu.SemaphoreType.DMA((share // BIAS_ROWS,)),
        ] + [pltpu.SemaphoreType.DMA((share // BIAS_ROWS, n_dev // 2))] * 4,
        compiler_params=pltpu.CompilerParams(
            dimension_semantics=('arbitrary',), vmem_limit_bytes=VMEM_BYTES, collective_id=0, has_side_effects=True),
        name='row_attention',
    )(e_t, mask, pair, w_pair_t, w_in, w_out)


def col_kernel(n_heads, r_ref, m_ref, wc_ref, wco_ref, wti_ref, wto_ref, o_ref):
    n_dev, n_i, half, lanes = r_ref.shape
    chans = lanes // 2
    width = wco_ref.shape[0]
    d = width // n_heads
    eye = jnp.where(lax.broadcasted_iota(jnp.int32, (lanes, lanes), 0) == lax.broadcasted_iota(jnp.int32, (lanes, lanes), 1),
                    1.0, 0.0).astype(BF)
    low = lax.broadcasted_iota(jnp.int32, (chans, 2 * half), 1) < half
    same_head = (lax.broadcasted_iota(jnp.int32, (width, width), 0) // d
                 == lax.broadcasted_iota(jnp.int32, (width, width), 1) // d)
    w_t = wc_ref[...].astype(F32).T
    wc = jnp.concatenate([w_t[:width]] + [w_t[width:width + d]] * n_heads + [w_t[width + d:width + 2 * d]] * n_heads
                         + [w_t[width + 2 * d:]], axis=0).astype(BF)
    wco, wti, wto = transposed(wco_ref[...]), transposed(wti_ref[...]), wto_ref[...]
    state = [dict() for _ in range(n_i)]

    def turn(i):
        state[i]['turned'] = dot_nt(eye, r_ref[:, i].reshape(n_dev * half, lanes))

    def project(i):
        s = state[i]
        turned = s.pop('turned')
        cols = []
        for n in range(n_dev // 2):
            a = turned[:chans, n * 2 * half:(n + 1) * 2 * half]
            b = turned[chans:, n * 2 * half:(n + 1) * 2 * half]
            cols.append(jnp.where(low, a, pltpu.roll(b, half, 1)))
            cols.append(jnp.where(low, pltpu.roll(a, half, 1), b))
        s['x'] = jnp.concatenate(cols, axis=1)
        s['proj'] = dot(wc, norm_rows(s['x'])).astype(BF)

    def q_mean(i):
        s = state[i]
        m = m_ref[pl.ds(i, 1), :]
        q_sum = jnp.sum(s['proj'][:width].astype(F32) * m, axis=1, keepdims=True)
        count = jnp.sum(m, axis=1, keepdims=True)
        mean = jnp.broadcast_to(q_sum / (count + MEAN_EPS), (width, width))
        s['q_rows'] = jnp.where(same_head, mean.T, 0.0).astype(BF)

    def logits(i):
        s = state[i]
        s['logits'] = dot(s.pop('q_rows'), s['proj'][width:2 * width])

    def softmax(i):
        s = state[i]
        proj = s.pop('proj')
        t = s.pop('logits') * (d ** -0.5) + MASK_BIG * (m_ref[pl.ds(i, 1), :] - 1.0)
        e = jnp.exp(t - jnp.max(t, axis=1, keepdims=True))
        den = jnp.sum(e, axis=1, keepdims=True)
        num = jnp.sum(e * proj[2 * width:3 * width].astype(F32), axis=1, keepdims=True)
        s['gated'] = (jax.nn.sigmoid(proj[3 * width:].astype(F32)) * (num / den)).astype(BF)

    def out(i):
        s = state[i]
        s['e2'] = (s.pop('x') + dot(wco, s.pop('gated'))).astype(BF)

    def hidden(i):
        s = state[i]
        s['hidden'] = jnp.maximum(dot(wti, norm_rows(s['e2'].astype(F32))), 0.0).astype(BF)

    def finish(i):
        s = state[i]
        o_ref[i] = (s.pop('e2').astype(F32) + dot(wto, s.pop('hidden'))).astype(BF)

    stages = dict(turn=turn, project=project, q_mean=q_mean, logits=logits, softmax=softmax, out=out, hidden=hidden, finish=finish)
    for step in range(n_i + max(lag for _, lag in COL_STAGES)):
        for name, lag in COL_STAGES:
            if 0 <= step - lag < n_i:
                stages[name](step - lag)


def column_and_transition(n_heads, received, mask, wc, wco, wti, wto):
    n_dev, share, half, lanes = received.shape
    n_seq = mask.shape[1]

    def whole(a):
        return pl.BlockSpec(a.shape, lambda n: (0,) * a.ndim)

    return pl.pallas_call(
        functools.partial(col_kernel, n_heads),
        grid=(share // TILE_RES,),
        in_specs=[
            pl.BlockSpec((n_dev, TILE_RES, half, lanes), lambda n: (0, n, 0, 0)),
            pl.BlockSpec((TILE_RES, n_seq), lambda n: (n, 0)),
            whole(wc), whole(wco), whole(wti), whole(wto),
        ],
        out_specs=pl.BlockSpec((TILE_RES, lanes // 2, n_seq), lambda n: (n, 0, 0)),
        out_shape=jax.ShapeDtypeStruct((share, lanes // 2, n_seq), BF),
        compiler_params=pltpu.CompilerParams(dimension_semantics=('arbitrary',), vmem_limit_bytes=VMEM_BYTES),
        name='column_and_transition',
    )(received, mask, wc, wco, wti, wto)


def solution(mesh):
    n_dev = mesh.shape['seq']

    def local_block(msa, mask, pair, w_pair_bias, w_row_in, w_row_out, w_col_in, w_col_out, w_trans_in, w_trans_out):
        n_heads = w_pair_bias.shape[1]
        received, mask_cols = row_attention(
            n_dev, jnp.transpose(msa, (0, 2, 1)), mask, pair, w_pair_bias.T, w_row_in, w_row_out)
        out = column_and_transition(n_heads, received, mask_cols, w_col_in, w_col_out, w_trans_in, w_trans_out.T)
        return jnp.transpose(out, (2, 0, 1))

    rows = P(('batch', 'seq'))
    return jax.shard_map(local_block, mesh=mesh, in_specs=(rows, rows, rows) + (P(),) * 7, out_specs=P('batch', 'seq'),
                         check_vma=False)
```
